256 devices in a mesh: dp: 4 (over x), seq: 8 (over y, core), tp: 8 (over z).
Axes of the slice: x: 4, y: 4, z: 8, core: 2. Of those that a mesh axis runs over, the one named last changes fastest.
Arguments:
- queries: bfloat16 [16384, 4096], P(('dp', 'seq'), 'tp'), parts along dimension 0, may hold values from -181 to 181
- rotated_key_states: bfloat16 [16384, 1024], P(('dp', 'seq'), 'tp'), parts along dimension 0, may hold values from -6.1 to 6.1
- value_state_vectors: bfloat16 [16384, 1024], P(('dp', 'seq'), 'tp'), parts along dimension 0, may hold values from -6 to 6
- out_weight: bfloat16 [4096, 8192], P('tp'), may hold values from -0.15625 to 0.15625
- residual: bfloat16 [16384, 8192], P(('dp', 'seq', 'tp')), parts along dimension 0, may hold values from -0.75 to 0.75
- norm_gain: bfloat16 [8192], replicated, may hold values from 0.099609375 to 2
Outputs:
- new_residual: bfloat16 [16384, 8192], P(('dp', 'seq', 'tp')), parts along dimension 0
- next_input: bfloat16 [16384, 8192], P(('dp', 'seq', 'tp')), parts along dimension 0
The draws below stay inside these ranges and needn't reach their ends.
There are 4 independent parts, one for each index of `dp`. The reference program is written for one: setup_inputs(seed, part) draws one part's arguments, and reference() takes and returns one part's arrays. A program takes and returns all parts, laid end to end along the dimension named above; an argument that names none is the same for every part. Nothing has to cross between parts.
All inputs are finite; a program needn't handle non-finite values.
Results may differ from the reference program's by a relative error of at most 0.025.
Values may be sent and summed in bfloat16 or wider, within the bound.
A program may use at most 192 MiB of HBM per device.

```python
import math
import jax
import jax.numpy as jnp
from jax import lax

D = 8192
HEAD_SIZE = 128
HQ_DEV = 4
QUERY_HEADS = 32
KEY_VALUE_HEADS = 8
SEQUENCE_TOKENS = 4096
N_TP = 8


def drawn_pair(key):
    query_key = jax.random.fold_in(key, 11)
    random_key_for_keys = jax.random.fold_in(key, 12)
    query_rows = 1.2 * jnp.clip(jax.random.normal(query_key, (SEQUENCE_TOKENS, QUERY_HEADS * HEAD_SIZE), jnp.float32), -5.0, 5.0)
    key_row_block = 1.2 * jnp.clip(jax.random.normal(random_key_for_keys, (SEQUENCE_TOKENS, KEY_VALUE_HEADS * HEAD_SIZE), jnp.float32), -5.0, 5.0)
    return (query_rows, key_row_block)


def draw_queries(key, part):
    return drawn_pair(key)[0].astype(jnp.bfloat16)


def draw_rotated_key_states(key, part):
    return drawn_pair(key)[1].astype(jnp.bfloat16)


def draw_out_weight(key, part):
    row_total = QUERY_HEADS * HEAD_SIZE
    entry_key = jax.random.fold_in(key, 31)
    factor_key = jax.random.fold_in(key, 32)
    entries = jnp.clip(jax.random.normal(entry_key, (row_total // 16, 16, D), jnp.float32), -5.0, 5.0)
    exponents = jax.random.uniform(factor_key, (row_total // 16, 1, D), jnp.float32, jnp.log(1.0 / 16.0), 0.0)
    factors = jnp.exp(exponents)
    group_count = QUERY_HEADS // HQ_DEV
    block_index = jnp.arange(row_total // 16, dtype=jnp.int32)
    group_index = block_index * 16 // (HQ_DEV * HEAD_SIZE)
    group_frac = group_index.astype(jnp.float32) / max(group_count - 1, 1)
    group_scale = jnp.exp(jnp.log(4.0) * (group_frac - 1.0)).reshape(row_total // 16, 1, 1)
    scaled = entries * factors * group_scale * (2.0 / row_total ** 0.5)
    return scaled.reshape(row_total, D).astype(jnp.bfloat16)


def block_levels(own_key, shape, cuts, low, top_value):
    loudness, own = 1.0, jax.random.fold_in(own_key, 6)
    for dim, shards_of in cuts:
        heights = jnp.exp(jax.random.uniform(jax.random.fold_in(own, dim), (shards_of,), jnp.float32, low / len(cuts), top_value / len(cuts)))
        loudness = loudness * jnp.repeat(heights, shape[dim] // shards_of).reshape([-1 if axis == dim else 1 for axis in range(len(shape))])
    return loudness


def gaussian(own_key, extent, scale, reach, cuts=(), kind=jnp.bfloat16):
    level = block_levels(own_key, extent, cuts, -0.22, 0.18) if cuts else 1.0
    array = jax.random.normal(own_key, extent, jnp.float32) * scale * level
    return jnp.minimum(jnp.maximum(array, -reach), reach).astype(kind)


def setup_inputs(seed: int = 0, part: int = 0) -> dict:
    arg_keys = jax.random.split(jax.random.key(seed), 7)
    own_keys = jax.random.split(jax.random.fold_in(arg_keys[6], part), 7)
    return {
        "queries": draw_queries(jax.random.fold_in(jax.random.fold_in(arg_keys[6], part), 71), part),
        "rotated_key_states": draw_rotated_key_states(jax.random.fold_in(jax.random.fold_in(arg_keys[6], part), 71), part),
        "value_state_vectors": gaussian(own_keys[2], (SEQUENCE_TOKENS, KEY_VALUE_HEADS * HEAD_SIZE), 1.0, 6.0, ((0, 8), (1, 8))),
        "out_weight": draw_out_weight(jax.random.fold_in(arg_keys[6], 71), part),
        "residual": gaussian(own_keys[4], (SEQUENCE_TOKENS, D), 0.05, 0.75, ((0, 64),)),
        "norm_gain": jnp.clip(jnp.exp(jax.random.uniform(arg_keys[5], (D,), jnp.float32, math.log(0.099609375), math.log(2.0))), 0.099609375, 2.0).astype(jnp.bfloat16),
    }


softness = 0.9
scale_floor = 256.0

def soft_grid(values):
    return values - softness * jnp.sin(jnp.pi * values) / jnp.pi

def fake_quant(blocks, block_axis, peak):
    block_max = lax.optimization_barrier(jnp.max(jnp.abs(blocks), axis=block_axis, keepdims=True))
    tensor_scale = peak / (6.0 * 448.0)
    block_scale = jnp.maximum(block_max / (6.0 * tensor_scale), scale_floor).astype(jnp.bfloat16)
    block_scale = lax.optimization_barrier(block_scale).astype(jnp.float32)
    spacing = block_scale * tensor_scale
    payload = soft_grid(blocks / spacing).astype(jnp.bfloat16)
    payload = lax.optimization_barrier(payload).astype(jnp.float32)
    return (payload * spacing).astype(jnp.bfloat16)

def reference(queries, rotated_key_states, value_state_vectors, out_weight, residual, norm_gain):
    score_scale = HEAD_SIZE ** (-0.5)
    grouped_heads = QUERY_HEADS // KEY_VALUE_HEADS
    q_heads = queries.reshape(SEQUENCE_TOKENS, QUERY_HEADS, HEAD_SIZE)
    key_heads = rotated_key_states.reshape(SEQUENCE_TOKENS, KEY_VALUE_HEADS, HEAD_SIZE)
    value_heads = value_state_vectors.reshape(SEQUENCE_TOKENS, KEY_VALUE_HEADS, HEAD_SIZE)
    positions = jnp.arange(SEQUENCE_TOKENS, dtype=jnp.int32)
    allowed = positions[:, None] >= positions[None, :]

    def one_head(head_index):
        q_one = lax.dynamic_index_in_dim(q_heads, head_index, 1, keepdims=False)
        kv_index = head_index // grouped_heads
        k_one = lax.dynamic_index_in_dim(key_heads, kv_index, 1, keepdims=False)
        v_one = lax.dynamic_index_in_dim(value_heads, kv_index, 1, keepdims=False)
        scores = jnp.dot(q_one, k_one.T, preferred_element_type=jnp.float32) * score_scale
        scores = jnp.where(allowed, scores, -jnp.inf)
        row_top = lax.optimization_barrier(jnp.max(scores, axis=1, keepdims=True))
        weights = jnp.exp(scores - row_top)
        totals = lax.optimization_barrier(jnp.sum(weights, axis=1, keepdims=True))
        attended = jnp.dot(weights.astype(jnp.bfloat16), v_one, preferred_element_type=jnp.float32) / totals
        return attended.astype(jnp.bfloat16)
    attended = lax.map(one_head, jnp.arange(QUERY_HEADS, dtype=jnp.int32))
    features = QUERY_HEADS * HEAD_SIZE
    act_t = attended.transpose(0, 2, 1).reshape(features, SEQUENCE_TOKENS).astype(jnp.float32)
    act_peak = jnp.max(jnp.abs(act_t))
    act_q = fake_quant(act_t.reshape(features // 16, 16, SEQUENCE_TOKENS), 1, act_peak).reshape(features, SEQUENCE_TOKENS)
    weight_f = out_weight.astype(jnp.float32)
    weight_peak = jnp.max(jnp.abs(weight_f))
    weight_q = fake_quant(weight_f.reshape(features // 16, 16, D), 1, weight_peak).reshape(features, D)
    group_width = features // N_TP
    projected = jnp.zeros((SEQUENCE_TOKENS, D), jnp.float32)
    for group_rank in range(N_TP):
        lower = group_rank * group_width
        partial_sum = lax.dot_general(act_q[lower:lower + group_width], weight_q[lower:lower + group_width], (((0,), (0,)), ((), ())), preferred_element_type=jnp.float32)
        partial_sum = lax.optimization_barrier(partial_sum.astype(jnp.bfloat16)).astype(jnp.float32)
        projected = projected + partial_sum
    hidden_sum = residual.astype(jnp.float32) + projected
    new_residual = hidden_sum.astype(jnp.bfloat16)
    mean_square = lax.optimization_barrier(jnp.mean(hidden_sum * hidden_sum, axis=1, keepdims=True))
    normed = hidden_sum * lax.rsqrt(mean_square + 1e-05) * norm_gain.astype(jnp.float32)
    norm_peak = jnp.max(jnp.abs(normed))
    next_input = fake_quant(normed.reshape(SEQUENCE_TOKENS, D // 16, 16), 2, norm_peak).reshape(SEQUENCE_TOKENS, D)
    return (new_residual, next_input)
```

```python
import jax
import jax.numpy as jnp
from jax import lax
from jax.experimental import pallas as pl
from jax.experimental.pallas import tpu as pltpu
from jax.sharding import PartitionSpec as P

D = 8192
HEAD = 128
SOFT = 0.9
FLOOR = 256.0
NEG = -1e30
MESH = pl.DeviceIdType.MESH
F32 = jnp.float32
BF16 = jnp.bfloat16

TOK = 512
HEADS = 4
FEAT = HEADS * HEAD
NTP = 8
NSEQ = 8
NDP = 4
OWN = TOK // NTP
COLS = D // NSEQ
SUB = COLS // NDP
RA = 368
SCALE = HEAD ** (-0.5) * 1.4426950408889634

QCO = (
    -0.00012284770491532981,
    0.00218366552144289,
    -0.02393284998834133,
    0.16680589318275452,
    -0.6449338793754578,
    1.0,
)


def soft_grid(u):
    w = u - 2.0 * jnp.round(u * 0.5)
    z = w * w
    q = jnp.full_like(z, QCO[0])
    for co in QCO[1:]:
        q = q * z + co
    return u - SOFT * (w * ((1.0 - z) * q))


def quantized(x, block_max, peak):
    tensor_scale = peak / (6.0 * 448.0)
    block_scale = jnp.maximum(block_max / (6.0 * tensor_scale), FLOOR).astype(BF16).astype(F32)
    spacing = block_scale * tensor_scale
    payload = soft_grid(x / spacing).astype(BF16).astype(F32)
    return (payload * spacing).astype(BF16)


def lane_block_max(x):
    for sh in (1, 2, 4, 8):
        x = jnp.maximum(x, pltpu.roll(x, sh, 1))
    lane = lax.broadcasted_iota(jnp.int32, x.shape, 1)
    x = jnp.where(lane % 16 == 15, x, 0.0)
    for sh in (1, 2, 4, 8):
        x = jnp.maximum(x, pltpu.roll(x, 128 - sh, 1))
    return x


class Copies:
    def __init__(self, send_sems, recv_sems):
        self.send_sems, self.recv_sems, self.started = send_sems, recv_sems, []

    def start(self, src, dst, dev, landing):
        i = len(self.started)
        out = pltpu.make_async_remote_copy(
            src_ref=src,
            dst_ref=dst,
            send_sem=self.send_sems.at[i],
            recv_sem=self.recv_sems.at[i],
            device_id=dev,
            device_id_type=MESH,
        )
        out.start()
        back = pltpu.make_async_remote_copy(
            src_ref=landing,
            dst_ref=landing,
            send_sem=self.send_sems.at[i],
            recv_sem=self.recv_sems.at[i],
            device_id=dev,
            device_id_type=MESH,
        )
        self.started.append(out)
        return back

    def finish(self):
        for out in self.started:
            out.wait_send()


N_COPIES = 160


def kernel(
    q_hbm,
    k_hbm,
    v_hbm,
    w_hbm,
    res_hbm,
    gain_ref,
    new_ref,
    next_ref,
    q_buf,
    kv_buf,
    w_stage,
    w_slice,
    w_all,
    vt_buf,
    m_ref,
    l_ref,
    o_ref,
    att_buf,
    z_buf,
    act_all,
    out_buf,
    part_buf,
    res_buf,
    hid_buf,
    tiles,
    send_sems,
    recv_sems,
    local_sems,
):
    dd, ss, tt = lax.axis_index("dp"), lax.axis_index("seq"), lax.axis_index("tp")
    yy = lax.div(ss, 2)
    cc = ss - 2 * yy

    def sid(dy, dc):
        return lax.rem(yy + dy + 4, 4) * 2 + (cc if dc == 0 else 1 - cc)

    def zt(k):
        return lax.rem(tt + k + 2 * NTP, NTP)

    def sq(k):
        return lax.rem(ss + k + 2 * NSEQ, NSEQ)

    def xd(k):
        return lax.rem(dd + k + 2 * NDP, NDP)

    loads = [
        pltpu.make_async_copy(k_hbm, kv_buf.at[ss, 0], local_sems.at[0]),
        pltpu.make_async_copy(v_hbm, kv_buf.at[ss, 1], local_sems.at[1]),
        pltpu.make_async_copy(q_hbm, q_buf, local_sems.at[2]),
        pltpu.make_async_copy(
            w_hbm.at[:, pl.ds(pl.multiple_of(ss * COLS + dd * SUB, SUB), SUB)],
            w_slice,
            local_sems.at[3],
        ),
    ]
    for i in range(4):
        loads.append(
            pltpu.make_async_copy(
                w_hbm.at[pl.ds(i * 128, 128)], w_stage.at[pl.ds(i * 128, 128)], local_sems.at[4 + i]
            )
        )
    loads.append(pltpu.make_async_copy(res_hbm, res_buf, local_sems.at[8]))
    for load in loads:
        load.start()

    barrier = pltpu.get_barrier_semaphore()
    for k in range(1, NTP):
        pl.semaphore_signal(barrier, inc=1, device_id={"tp": zt(k)}, device_id_type=MESH)
    for k in range(1, NSEQ):
        pl.semaphore_signal(barrier, inc=1, device_id={"seq": sq(k)}, device_id_type=MESH)
    for k in (1, 3):
        pl.semaphore_signal(barrier, inc=1, device_id={"dp": xd(k)}, device_id_type=MESH)
    pl.semaphore_wait(barrier, NTP - 1 + NSEQ - 1 + 2)

    copies = Copies(send_sems, recv_sems)

    class SeqGather:
        def __init__(self, unit, half):
            self.unit, self.half = unit, half
            own = unit(sid(0, 0))
            self.x1 = copies.start(own, own, {"seq": sid(1, 0)}, unit(sid(-1, 0)))
            self.x2 = copies.start(own, own, {"seq": sid(-1, 0)}, unit(sid(1, 0)))
            self.x0 = copies.start(own, own, {"seq": sid(0, 1)}, unit(sid(0, 1)))

        def low(self):
            self.x1.wait_recv()
            got, part = self.unit(sid(-1, 0)), self.half(sid(-1, 0), 0)
            self.x4 = copies.start(part, part, {"seq": sid(1, 0)}, self.half(sid(2, 0), 0))
            self.x3 = copies.start(got, got, {"seq": sid(0, 1)}, self.unit(sid(-1, 1)))

        def high(self):
            self.x2.wait_recv()
            got, part = self.unit(sid(1, 0)), self.half(sid(1, 0), 1)
            self.x6 = copies.start(part, part, {"seq": sid(-1, 0)}, self.half(sid(2, 0), 1))
            self.x5 = copies.start(got, got, {"seq": sid(0, 1)}, self.unit(sid(1, 1)))

        def far(self):
            self.x4.wait_recv()
            self.x6.wait_recv()
            got = self.unit(sid(2, 0))
            self.x7 = copies.start(got, got, {"seq": sid(0, 1)}, self.unit(sid(2, 1)))

    def spread_tile(src, dst_of, axis, at):
        me = tt if axis == "tp" else ss
        return [
            copies.start(tiles.at[src], tiles.at[dst_of + me], {axis: at(k)}, tiles.at[dst_of + at(-k)])
            for k in range(1, 8)
        ]

    def max_of_tiles(first):
        top = tiles[first]
        for i in range(1, 8):
            top = jnp.maximum(top, tiles[first + i])
        return top

    loads[0].wait()
    loads[1].wait()
    kv = SeqGather(lambda i: kv_buf.at[i], lambda i, h: kv_buf.at[i, h])

    tiles[48] = jnp.zeros((8, 128), F32)
    for i in range(4):
        loads[4 + i].wait()

        @pl.loop(0, 16)
        def _(j, i=i):
            top = tiles[48]
            piece = jnp.abs(w_stage[i * 128 : (i + 1) * 128, pl.ds(pl.multiple_of(j * 512, 512), 512)].astype(F32))
            top4 = jnp.max(piece.reshape(16, 8, 512), axis=0)
            for n in range(4):
                top = jnp.maximum(top, top4[:, n * 128 : (n + 1) * 128])
            tiles[48] = top

    tiles[8 + tt] = tiles[48]
    w_top = spread_tile(48, 8, "tp", zt)

    def attend(block, kind):
        k_blk = kv_buf[block, 0]
        vt_buf[...] = kv_buf[block, 1].T

        @pl.loop(0, HEADS)
        def _(h):
            q_h = q_buf[:, pl.ds(pl.multiple_of(h * HEAD, HEAD), HEAD)]
            sc = lax.dot_general(k_blk, q_h, (((1,), (1,)), ((), ())), preferred_element_type=F32)
            if kind == "own":
                key = lax.broadcasted_iota(jnp.int32, (TOK, TOK), 0)
                query = lax.broadcasted_iota(jnp.int32, (TOK, TOK), 1)
                sc = jnp.where(key <= query, sc, NEG)
            top = jnp.max(sc, axis=0, keepdims=True)
            if kind != "own":
                old = m_ref[h]
                top = jnp.maximum(old, top)
            p = jnp.exp2((sc - top) * SCALE)
            total = jnp.sum(p, axis=0, keepdims=True)
            o = lax.dot_general(
                vt_buf[...], p.astype(BF16), (((1,), (0,)), ((), ())), preferred_element_type=F32
            )
            if kind != "own":
                shrink = jnp.exp2((old - top) * SCALE)
                total = total + l_ref[h] * shrink
                o = o + o_ref[h] * shrink
            m_ref[h] = top
            l_ref[h] = total
            o_ref[h] = o

    def attend_if_before(block):
        @pl.when(block < ss)
        def _():
            attend(block, "before")

    loads[2].wait()
    attend(ss, "own")

    loads[3].wait()
    for cp in w_top:
        cp.wait_recv()
    w_peak = jnp.max(max_of_tiles(8))

    @pl.loop(0, 8)
    def _(i):
        rows = pl.ds(pl.multiple_of(i * 64, 64), 64)
        x = w_slice[rows, :].astype(F32).reshape(4, 16, SUB)
        top = jnp.max(jnp.abs(x), axis=1, keepdims=True)
        top = jnp.broadcast_to(top, x.shape)
        w_all[dd, pl.ds(pl.multiple_of(tt * FEAT + i * 64, 64), 64), :] = quantized(x, top, w_peak).reshape(64, SUB)

    def unit_a(d, t):
        return w_all.at[d, pl.ds(pl.multiple_of(t * FEAT, 16), RA)]

    def unit_b(d, t):
        return w_all.at[d, pl.ds(pl.multiple_of(t * FEAT + RA, 16), FEAT - RA)]

    def bundle_b(t):
        return w_all.at[:, pl.ds(pl.multiple_of(t * FEAT + RA, 16), FEAT - RA)]

    rel = (0, -1, 1, -2, 2, -3, 3, -4)
    up = {0: 0, 1: 1, 2: 3, 3: 5, 4: 7}
    down = {0: 0, 1: 2, 2: 4, 3: 6}
    x_left, x_right, x_far, b_up, b_down, a_up, a_down = {}, {}, {}, {}, {}, {}, {}

    def x_sends(j):
        t_j = zt(rel[j])
        own = unit_a(dd, t_j)
        x_left[j] = copies.start(own, own, {"dp": xd(1)}, unit_a(xd(-1), t_j))
        x_right[j] = copies.start(own, own, {"dp": xd(-1)}, unit_a(xd(1), t_j))

    def a_send_up(step):
        u = unit_a(dd, zt(-step))
        a_up[step + 1] = copies.start(u, u, {"tp": zt(1)}, unit_a(dd, zt(-step - 1)))

    def a_send_down(step):
        u = unit_a(dd, zt(step))
        a_down[step + 1] = copies.start(u, u, {"tp": zt(-1)}, unit_a(dd, zt(step + 1)))

    def b_send_up(step):
        u = bundle_b(zt(-step))
        b_up[step + 1] = copies.start(u, u, {"tp": zt(1)}, bundle_b(zt(-step - 1)))

    def b_send_down(step):
        u = bundle_b(zt(step))
        b_down[step + 1] = copies.start(u, u, {"tp": zt(-1)}, bundle_b(zt(step + 1)))

    own_b = unit_b(dd, tt)
    bx_left = copies.start(own_b, own_b, {"dp": xd(1)}, unit_b(xd(-1), tt))
    bx_right = copies.start(own_b, own_b, {"dp": xd(-1)}, unit_b(xd(1), tt))
    a_send_up(0)
    a_send_down(0)
    x_sends(0)

    bx_far = []

    def ev_bx():
        bx_left.wait_recv()
        u = unit_b(xd(-1), tt)
        bx_far.append(copies.start(u, u, {"dp": xd(1)}, unit_b(xd(2), tt)))
        bx_right.wait_recv()

    def ev_b0():
        bx_far[0].wait_recv()
        b_send_up(0)
        b_send_down(0)

    def ev_a(step):
        def go():
            a_up[step].wait_recv()
            if step < 4:
                a_send_up(step)
            x_sends(up[step])
            if step < 4:
                a_down[step].wait_recv()
                if step < 3:
                    a_send_down(step)
                x_sends(down[step])

        return go

    def ev_b(step):
        def go():
            b_up[step].wait_recv()
            if step < 4:
                b_send_up(step)
            if step < 4:
                b_down[step].wait_recv()
                if step < 3:
                    b_send_down(step)

        return go

    def ev_x(j):
        def go():
            t_j = zt(rel[j])
            x_left[j].wait_recv()
            if j % 2 == 0:
                u = unit_a(xd(-1), t_j)
                x_far[j] = copies.start(u, u, {"dp": xd(1)}, unit_a(xd(2), t_j))
            x_right[j].wait_recv()
            if j % 2 == 1:
                u = unit_a(xd(1), t_j)
                x_far[j] = copies.start(u, u, {"dp": xd(-1)}, unit_a(xd(2), t_j))

        return go

    events = [
        ev_bx,
        ev_a(1),
        ev_b0,
        ev_x(0),
        ev_a(2),
        ev_x(1),
        ev_b(1),
        ev_x(2),
        ev_a(3),
        ev_x(3),
        ev_b(2),
        ev_a(4),
        ev_x(4),
        ev_b(3),
        ev_x(5),
        ev_x(6),
        ev_b(4),
        ev_x(7),
    ]
    done = [0]

    def progress(upto):
        while done[0] < min(upto, len(events)):
            events[done[0]]()
            done[0] += 1

    kv.x0.wait_recv()
    attend_if_before(sid(0, 1))
    kv.low()
    attend_if_before(sid(-1, 0))
    kv.high()
    progress(1)
    attend_if_before(sid(1, 0))
    kv.x3.wait_recv()
    attend_if_before(sid(-1, 1))
    kv.far()
    progress(2)
    kv.x5.wait_recv()
    attend_if_before(sid(1, 1))
    progress(4)
    attend_if_before(sid(2, 0))
    kv.x7.wait_recv()
    progress(5)
    attend_if_before(sid(2, 1))

    tiles[49] = jnp.zeros((8, 128), F32)
    for h in range(HEADS):
        a = (o_ref[h] / l_ref[h]).T.astype(BF16)
        att_buf[:, h * HEAD : (h + 1) * HEAD] = a
        tiles[49] = jnp.maximum(tiles[49], jnp.max(jnp.abs(a.astype(F32)).reshape(TOK // 8, 8, HEAD), axis=0))
    tiles[16 + tt] = tiles[49]
    a_moves = []
    for k in range(1, NTP):
        a_moves.append(
            copies.start(
                att_buf.at[pl.ds(pl.multiple_of(zt(k) * OWN, OWN), OWN)],
                z_buf.at[tt],
                {"tp": zt(k)},
                z_buf.at[zt(-k)],
            )
        )
    a_top = spread_tile(49, 16, "tp", zt)
    z_buf[tt] = att_buf[pl.ds(pl.multiple_of(tt * OWN, OWN), OWN), :]
    progress(9)
    for cp in a_top:
        cp.wait_recv()
    tiles[50] = max_of_tiles(16)
    tiles[24 + ss] = tiles[50]
    s_top = spread_tile(50, 24, "seq", sq)
    for cp in a_moves:
        cp.wait_recv()
    for cp in s_top:
        cp.wait_recv()
    a_peak = jnp.max(max_of_tiles(24))

    @pl.loop(0, NTP)
    def _(i):
        for n in range(FEAT // 128):
            x = z_buf[i, :, n * 128 : (n + 1) * 128].astype(F32)
            cols = pl.ds(pl.multiple_of(i * FEAT + n * 128, 128), 128)
            act_all[ss, :, cols] = quantized(x, lane_block_max(jnp.abs(x)), a_peak)

    act = SeqGather(lambda i: act_all.at[i], lambda i, h: act_all.at[i, pl.ds(h * (OWN // 2), OWN // 2)])
    progress(12)
    act.low()
    act.high()
    progress(14)
    act.x0.wait_recv()
    act.far()
    act.x3.wait_recv()
    act.x5.wait_recv()
    act.x7.wait_recv()
    progress(len(events))

    moves = []

    def project(d, last):
        lhs = act_all[...].reshape(NSEQ * OWN, NTP * FEAT)
        prod = jnp.dot(lhs, w_all[d], preferred_element_type=F32)
        out_buf[d] = prod.astype(BF16).reshape(NSEQ, OWN, SUB)
        for k in range(1, NSEQ):
            moves.append(
                copies.start(
                    out_buf.at[d, sq(k)], part_buf.at[ss, d], {"seq": sq(k)}, part_buf.at[sq(-k), d]
                )
            )
        part_buf[ss, d] = out_buf[d, ss]

    project(dd, False)
    project(xd(-1), False)
    project(xd(1), False)
    for j in range(8):
        x_far[j].wait_recv()
    project(xd(2), True)
    loads[8].wait()
    for cp in moves:
        cp.wait_recv()

    square = jnp.zeros((OWN, 128), F32)
    for i in range(NSEQ):
        for j in range(NDP):
            cols = slice(i * COLS + j * SUB, i * COLS + (j + 1) * SUB)
            hid = res_buf[:, cols].astype(F32) + part_buf[i, j].astype(F32)
            hid_buf[:, cols] = hid
            new_ref[:, cols] = hid.astype(BF16)
            sqr = hid * hid
            for n in range(SUB // 128):
                square = square + sqr[:, n * 128 : (n + 1) * 128]
    mean = jnp.sum(square, axis=1, keepdims=True) * (1.0 / D)
    root = lax.rsqrt(mean + 1e-05)
    top = jnp.zeros((OWN, 128), F32)
    for i in range(D // 128):
        cols = slice(i * 128, (i + 1) * 128)
        normed = hid_buf[:, cols] * root * gain_ref[:, cols].astype(F32)
        hid_buf[:, cols] = normed
        top = jnp.maximum(top, jnp.abs(normed))
    tiles[51] = jnp.max(top.reshape(OWN // 8, 8, 128), axis=0)
    tiles[32 + tt] = tiles[51]
    for cp in spread_tile(51, 32, "tp", zt):
        cp.wait_recv()
    tiles[52] = max_of_tiles(32)
    tiles[40 + ss] = tiles[52]
    for cp in spread_tile(52, 40, "seq", sq):
        cp.wait_recv()
    n_peak = jnp.max(max_of_tiles(40))

    @pl.loop(0, D // 256)
    def _(i):
        for n in range(2):
            cols = pl.ds(pl.multiple_of(i * 256 + n * 128, 128), 128)
            x = hid_buf[:, cols]
            next_ref[:, cols] = quantized(x, lane_block_max(jnp.abs(x)), n_peak)

    copies.finish()


def local(queries, keys, values, out_weight, residual, norm_gain):
    any_space = pl.BlockSpec(memory_space=pl.ANY)
    vmem = pl.BlockSpec(memory_space=pltpu.VMEM)
    out = jax.ShapeDtypeStruct((OWN, D), BF16)
    return pl.pallas_call(
        kernel,
        out_shape=(out, out),
        in_specs=[any_space] * 5 + [vmem],
        out_specs=(vmem, vmem),
        scratch_shapes=[
            pltpu.VMEM((TOK, FEAT), BF16),
            pltpu.VMEM((NSEQ, 2, TOK, HEAD), BF16),
            pltpu.VMEM((FEAT, D), BF16),
            pltpu.VMEM((FEAT, SUB), BF16),
            pltpu.VMEM((NDP, NTP * FEAT, SUB), BF16),
            pltpu.VMEM((HEAD, TOK), BF16),
            pltpu.VMEM((HEADS, 1, TOK), F32),
            pltpu.VMEM((HEADS, 1, TOK), F32),
            pltpu.VMEM((HEADS, HEAD, TOK), F32),
            pltpu.VMEM((TOK, FEAT), BF16),
            pltpu.VMEM((NTP, OWN, FEAT), BF16),
            pltpu.VMEM((NSEQ, OWN, NTP * FEAT), BF16),
            pltpu.VMEM((NDP, NSEQ, OWN, SUB), BF16),
            pltpu.VMEM((NSEQ, NDP, OWN, SUB), BF16),
            pltpu.VMEM((OWN, D), BF16),
            pltpu.VMEM((OWN, D), F32),
            pltpu.VMEM((56, 8, 128), F32),
            pltpu.SemaphoreType.DMA((N_COPIES,)),
            pltpu.SemaphoreType.DMA((N_COPIES,)),
            pltpu.SemaphoreType.DMA((9,)),
        ],
        compiler_params=pltpu.CompilerParams(
            collective_id=0, has_side_effects=True, vmem_limit_bytes=60 * 1024 * 1024
        ),
    )(queries, keys, values, out_weight, residual, norm_gain.reshape(1, D))


def solution(mesh):
    in_specs = (
        P(("dp", "seq"), "tp"),
        P(("dp", "seq"), "tp"),
        P(("dp", "seq"), "tp"),
        P("tp", None),
        P(("dp", "seq", "tp"), None),
        P(),
    )
    out_specs = (P(("dp", "seq", "tp"), None), P(("dp", "seq", "tp"), None))
    return jax.shard_map(local, mesh=mesh, in_specs=in_specs, out_specs=out_specs, check_vma=False)
```

```python
import jax
import jax.numpy as jnp
from jax import lax
from jax.experimental import pallas as pl
from jax.experimental.pallas import tpu as pltpu
from jax.sharding import PartitionSpec as P

D = 8192
HEAD = 128
FLOOR = 256.0
NEG = -1e30
MESH = pl.DeviceIdType.MESH
F32 = jnp.float32
BF16 = jnp.bfloat16

TOK = 512
HEADS = 4
FEAT = HEADS * HEAD
NTP = 8
NSEQ = 8
NDP = 4
OWN = TOK // NTP
COLS = D // NSEQ
SUB = COLS // NDP
PAIR = 2
HALF = OWN // 2
GROUP = 2
RA = 432
SCALE = HEAD ** (-0.5) * 1.4426950408889634

SINE = (
    -1.7606472969055176,
    5.904375076293945,
    -10.969871520996094,
    11.68786334991455,
    -5.921726226806641,
    0.8999996781349182,
)


def rounded(x, double):
    v = x / double
    f = v - jnp.round(v)
    z = f * f
    sine = SINE[0] * z + SINE[1]
    for co in SINE[2:]:
        sine = sine * z + co
    half = (v - f * sine).astype(BF16).astype(F32)
    return (half * double).astype(BF16)


def quantized_rows(x, peak):
    n, cols = x.shape
    x = x.reshape(n // 16, 16, cols)
    top = jnp.max(jnp.abs(x), axis=1, keepdims=True)
    tensor_scale = peak / (6.0 * 448.0)
    scale = jnp.maximum(top * (1.0 / (6.0 * tensor_scale)), FLOOR).astype(BF16).astype(F32)
    return rounded(x, jnp.broadcast_to(scale * (2.0 * tensor_scale), x.shape)).reshape(n, cols)


def quantized_lanes(pieces, peak, pick):
    rows = pieces[0].shape[0]
    tensor_scale = peak / (6.0 * 448.0)
    inverse = 1.0 / (6.0 * tensor_scale)
    scales = []
    for x in pieces:
        top = jnp.abs(x)
        for sh in (1, 2, 4, 8):
            top = jnp.maximum(top, pltpu.roll(top, sh, 1))
        scales.append(jnp.maximum(top * inverse, FLOOR).astype(BF16))
    spread = jnp.dot(jnp.concatenate(scales, axis=0), pick, preferred_element_type=F32)
    return [
        rounded(x, spread[i * rows : (i + 1) * rows] * (2.0 * tensor_scale)) for i, x in enumerate(pieces)
    ]


def pick_matrix():
    src = lax.broadcasted_iota(jnp.int32, (128, 128), 0)
    dst = lax.broadcasted_iota(jnp.int32, (128, 128), 1)
    same = (src // 16 == dst // 16) & (src % 16 == 15)
    return jnp.where(same, 1.0, 0.0).astype(BF16)


class Copies:
    def __init__(self, send_sems, recv_sems, dev):
        self.send_sems, self.recv_sems, self.dev = send_sems, recv_sems, dev
        self.sent, self.n_recv = [], 0

    def copy(self, src, dst, send, recv, dev):
        return pltpu.make_async_remote_copy(
            src_ref=src,
            dst_ref=dst,
            send_sem=self.send_sems.at[send],
            recv_sem=self.recv_sems.at[recv],
            device_id=dev,
            device_id_type=MESH,
        )

    def sender(self, total):
        self.sent.append(total)
        return len(self.sent) - 1

    def receiver(self):
        self.n_recv += 1
        return self.n_recv - 1

    def start(self, src, dst, dev, send, recv):
        self.copy(src, dst, send, recv, dev).start()

    def start_one(self, src, dst, dev, send, landing):
        recv = self.receiver()
        self.start(src, dst, dev, send, recv)
        return lambda: self.arrived(recv, landing)

    def arrived(self, recv, landing):
        self.copy(landing, landing, 0, recv, self.dev).wait_recv()

    def finish(self):
        for i, total in enumerate(self.sent):
            self.copy(total, total, i, 0, self.dev).wait_send()


N_SEND = 12
N_RECV = 73


def kernel(
    q_hbm,
    k_hbm,
    v_hbm,
    w_hbm,
    res_hbm,
    gain_ref,
    hid_ref,
    root_ref,
    top_ref,
    q_buf,
    kv_buf,
    w_stage,
    w_slice,
    w_all,
    vt_buf,
    m_ref,
    l_ref,
    o_ref,
    att_buf,
    z_buf,
    act_all,
    out_buf,
    part_buf,
    res_buf,
    hid_buf,
    tiles,
    pick_buf,
    root_buf,
    send_sems,
    recv_sems,
    local_sems,
):
    dd, ss, tt = lax.axis_index("dp"), lax.axis_index("seq"), lax.axis_index("tp")
    yy = lax.div(ss, 2)
    cc = ss - 2 * yy

    def sid(dy, dc):
        return lax.rem(yy + dy + 4, 4) * 2 + (cc if dc == 0 else 1 - cc)

    def zt(k):
        return lax.rem(tt + k + 2 * NTP, NTP)

    def sq(k):
        return lax.rem(ss + k + 2 * NSEQ, NSEQ)

    def xd(k):
        return lax.rem(dd + k + 2 * NDP, NDP)

    loads = [
        pltpu.make_async_copy(k_hbm, kv_buf.at[ss, 0], local_sems.at[0]),
        pltpu.make_async_copy(v_hbm, kv_buf.at[ss, 1], local_sems.at[1]),
        pltpu.make_async_copy(q_hbm, q_buf, local_sems.at[2]),
        pltpu.make_async_copy(
            w_hbm.at[:, pl.ds(pl.multiple_of(ss * COLS + dd * SUB, SUB), SUB)],
            w_slice,
            local_sems.at[3],
        ),
    ]
    for i in range(4):
        loads.append(
            pltpu.make_async_copy(
                w_hbm.at[pl.ds(i * 128, 128)], w_stage.at[pl.ds(i * 128, 128)], local_sems.at[4 + i]
            )
        )
    loads.append(pltpu.make_async_copy(res_hbm, res_buf, local_sems.at[8]))
    for load in loads:
        load.start()

    barrier = pltpu.get_barrier_semaphore()
    for k in range(1, NTP):
        pl.semaphore_signal(barrier, inc=1, device_id={"tp": zt(k)}, device_id_type=MESH)
    for k in range(1, NSEQ):
        pl.semaphore_signal(barrier, inc=1, device_id={"seq": sq(k)}, device_id_type=MESH)
    for k in (1, 3):
        pl.semaphore_signal(barrier, inc=1, device_id={"dp": xd(k)}, device_id_type=MESH)
    pl.semaphore_wait(barrier, NTP - 1 + NSEQ - 1 + 2)

    copies = Copies(send_sems, recv_sems, {"tp": zt(1)})
    pick_buf[...] = pick_matrix()

    class SeqGather:
        def __init__(self, unit, half, total):
            self.unit, self.half, self.send = unit, half, copies.sender(total)
            own = unit(sid(0, 0))
            self.x1 = self.go(own, sid(1, 0), unit(sid(-1, 0)))
            self.x2 = self.go(own, sid(-1, 0), unit(sid(1, 0)))
            self.x0 = self.go(own, sid(0, 1), unit(sid(0, 1)))

        def go(self, ref, to, landing):
            return copies.start_one(ref, ref, {"seq": to}, self.send, landing)

        def low(self):
            self.x1()
            got, part = self.unit(sid(-1, 0)), self.half(sid(-1, 0), 0)
            self.x4 = self.go(part, sid(1, 0), self.half(sid(2, 0), 0))
            self.x3 = self.go(got, sid(0, 1), self.unit(sid(-1, 1)))

        def high(self):
            self.x2()
            got, part = self.unit(sid(1, 0)), self.half(sid(1, 0), 1)
            self.x6 = self.go(part, sid(-1, 0), self.half(sid(2, 0), 1))
            self.x5 = self.go(got, sid(0, 1), self.unit(sid(1, 1)))

        def far(self):
            self.x4()
            self.x6()
            self.x7 = self.go(self.unit(sid(2, 0)), sid(0, 1), self.unit(sid(2, 1)))

    def spread_tile(src, dst_of, axis, at):
        me = tt if axis == "tp" else ss
        seven = tiles.at[pl.ds(dst_of, 7)]
        send, recv = copies.sender(seven), copies.receiver()
        for k in range(1, 8):
            copies.start(tiles.at[src], tiles.at[dst_of + me], {axis: at(k)}, send, recv)
        return lambda: copies.arrived(recv, seven)

    def max_of_tiles(first):
        top = tiles[first]
        for i in range(1, 8):
            top = jnp.maximum(top, tiles[first + i])
        return top

    loads[0].wait()
    loads[1].wait()
    kv = SeqGather(lambda i: kv_buf.at[i], lambda i, h: kv_buf.at[i, h], kv_buf.at[pl.ds(0, NSEQ - 1)])

    tiles[48] = jnp.zeros((8, 128), F32)
    for i in range(4):
        loads[4 + i].wait()

        @pl.loop(0, 16)
        def _(j, i=i):
            top = tiles[48]
            piece = jnp.abs(w_stage[i * 128 : (i + 1) * 128, pl.ds(pl.multiple_of(j * 512, 512), 512)].astype(F32))
            top4 = jnp.max(piece.reshape(16, 8, 512), axis=0)
            for n in range(4):
                top = jnp.maximum(top, top4[:, n * 128 : (n + 1) * 128])
            tiles[48] = top

    tiles[8 + tt] = tiles[48]
    w_top = spread_tile(48, 8, "tp", zt)

    def attend(block, kind):
        vt_buf[...] = kv_buf[block, 1].T

        @pl.loop(0, HEADS // PAIR)
        def _(i):
            heads = [i * PAIR + n for n in range(PAIR)]
            scores = [
                lax.dot_general(
                    kv_buf[block, 0],
                    q_buf[:, pl.ds(pl.multiple_of(h * HEAD, HEAD), HEAD)],
                    (((1,), (1,)), ((), ())),
                    preferred_element_type=F32,
                )
                for h in heads
            ]
            for h, sc in zip(heads, scores):
                if kind == "own":
                    key = lax.broadcasted_iota(jnp.int32, (TOK, TOK), 0)
                    query = lax.broadcasted_iota(jnp.int32, (TOK, TOK), 1)
                    sc = jnp.where(key <= query, sc, NEG)
                top = jnp.max(sc, axis=0, keepdims=True)
                if kind != "own":
                    old = m_ref[h]
                    top = jnp.maximum(old, top)
                p = jnp.exp2((sc - top) * SCALE)
                total = jnp.sum(p, axis=0, keepdims=True)
                o = lax.dot_general(
                    vt_buf[...], p.astype(BF16), (((1,), (0,)), ((), ())), preferred_element_type=F32
                )
                if kind != "own":
                    shrink = jnp.exp2((old - top) * SCALE)
                    total = total + l_ref[h] * shrink
                    o = o + o_ref[h] * shrink
                m_ref[h] = top
                l_ref[h] = total
                o_ref[h] = o

    def attend_if_before(block):
        @pl.when(block < ss)
        def _():
            attend(block, "before")

    loads[2].wait()
    attend(ss, "own")

    loads[3].wait()
    w_top()
    w_peak = jnp.max(max_of_tiles(8))

    @pl.loop(0, 8)
    def _(i):
        rows = pl.ds(pl.multiple_of(i * 64, 64), 64)
        w_all[dd, pl.ds(pl.multiple_of(tt * FEAT + i * 64, 64), 64), :] = quantized_rows(
            w_slice[rows, :].astype(F32), w_peak
        )

    def unit_a(d, t):
        return w_all.at[d, pl.ds(pl.multiple_of(t * FEAT, 16), RA)]

    def unit_b(d, t):
        return w_all.at[d, pl.ds(pl.multiple_of(t * FEAT + RA, 16), FEAT - RA)]

    def bundle_b(t):
        return w_all.at[:, pl.ds(pl.multiple_of(t * FEAT + RA, 16), FEAT - RA)]

    rel = (0, -1, 1, -2, 2, -3, 3, -4)
    up = {0: 0, 1: 1, 2: 3, 3: 5, 4: 7}
    down = {0: 0, 1: 2, 2: 4, 3: 6}
    x_left, x_right, x_far, b_up, b_down, a_up, a_down = {}, {}, {}, {}, {}, {}, {}

    w_send = copies.sender(w_all.at[:, pl.ds(0, 31 * FEAT // NDP)])

    def w_go(ref, to, landing):
        return copies.start_one(ref, ref, to, w_send, landing)

    def x_sends(j):
        t_j = zt(rel[j])
        own = unit_a(dd, t_j)
        x_left[j] = w_go(own, {"dp": xd(1)}, unit_a(xd(-1), t_j))
        x_right[j] = w_go(own, {"dp": xd(-1)}, unit_a(xd(1), t_j))

    def a_send_up(step):
        a_up[step + 1] = w_go(unit_a(dd, zt(-step)), {"tp": zt(1)}, unit_a(dd, zt(-step - 1)))

    def a_send_down(step):
        a_down[step + 1] = w_go(unit_a(dd, zt(step)), {"tp": zt(-1)}, unit_a(dd, zt(step + 1)))

    def b_send_up(step):
        b_up[step + 1] = w_go(bundle_b(zt(-step)), {"tp": zt(1)}, bundle_b(zt(-step - 1)))

    def b_send_down(step):
        b_down[step + 1] = w_go(bundle_b(zt(step)), {"tp": zt(-1)}, bundle_b(zt(step + 1)))

    own_b = unit_b(dd, tt)
    bx_left = w_go(own_b, {"dp": xd(1)}, unit_b(xd(-1), tt))
    bx_right = w_go(own_b, {"dp": xd(-1)}, unit_b(xd(1), tt))
    a_send_up(0)
    a_send_down(0)
    x_sends(0)

    bx_far = []

    def ev_bx():
        bx_left()
        bx_far.append(w_go(unit_b(xd(-1), tt), {"dp": xd(1)}, unit_b(xd(2), tt)))
        bx_right()

    def ev_b0():
        bx_far[0]()
        b_send_up(0)
        b_send_down(0)

    def ev_a(step):
        def go():
            a_up[step]()
            if step < 4:
                a_send_up(step)
            x_sends(up[step])
            if step < 4:
                a_down[step]()
                if step < 3:
                    a_send_down(step)
                x_sends(down[step])

        return go

    def ev_b(step):
        def go():
            b_up[step]()
            if step < 4:
                b_send_up(step)
                b_down[step]()
                if step < 3:
                    b_send_down(step)

        return go

    def ev_x(j):
        def go():
            t_j = zt(rel[j])
            x_left[j]()
            if j % 2 == 0:
                x_far[j] = w_go(unit_a(xd(-1), t_j), {"dp": xd(1)}, unit_a(xd(2), t_j))
            x_right[j]()
            if j % 2 == 1:
                x_far[j] = w_go(unit_a(xd(1), t_j), {"dp": xd(-1)}, unit_a(xd(2), t_j))

        return go

    events = [
        ev_bx,
        ev_a(1),
        ev_x(0),
        ev_b0,
        ev_a(2),
        ev_x(1),
        ev_x(2),
        ev_b(1),
        ev_a(3),
        ev_x(3),
        ev_b(2),
        ev_a(4),
        ev_x(4),
        ev_x(5),
        ev_b(3),
        ev_x(6),
        ev_x(7),
        ev_b(4),
    ]
    done = [0]

    def progress(upto):
        while done[0] < min(upto, len(events)):
            events[done[0]]()
            done[0] += 1

    kv.x0()
    attend_if_before(sid(0, 1))
    kv.low()
    attend_if_before(sid(-1, 0))
    kv.high()
    progress(2)
    attend_if_before(sid(1, 0))
    kv.x3()
    progress(4)
    attend_if_before(sid(-1, 1))
    kv.far()
    progress(5)
    kv.x5()
    attend_if_before(sid(1, 1))
    progress(6)
    attend_if_before(sid(2, 0))
    kv.x7()
    progress(8)
    attend_if_before(sid(2, 1))

    tiles[49] = jnp.zeros((8, 128), F32)
    for h in range(HEADS):
        a = (o_ref[h] / l_ref[h]).T.astype(BF16)
        att_buf[:, h * HEAD : (h + 1) * HEAD] = a
        tiles[49] = jnp.maximum(tiles[49], jnp.max(jnp.abs(a.astype(F32)).reshape(TOK // 8, 8, HEAD), axis=0))
    tiles[16 + tt] = tiles[49]
    a_top = spread_tile(49, 16, "tp", zt)
    a_moves = []
    for part in range(2):
        seven = z_buf.at[part, pl.ds(0, NTP - 1)]
        send, recv = copies.sender(seven), copies.receiver()
        for k in range(1, NTP):
            copies.start(
                att_buf.at[pl.ds(pl.multiple_of(zt(k) * OWN + part * HALF, HALF), HALF)],
                z_buf.at[part, tt],
                {"tp": zt(k)},
                send,
                recv,
            )
        a_moves.append(lambda recv=recv, seven=seven: copies.arrived(recv, seven))
        z_buf[part, tt] = att_buf[pl.ds(pl.multiple_of(tt * OWN + part * HALF, HALF), HALF), :]
    progress(10)
    a_top()
    tiles[50] = max_of_tiles(16)
    tiles[24 + ss] = tiles[50]
    s_top = spread_tile(50, 24, "seq", sq)
    progress(12)
    s_top()
    a_peak = jnp.max(max_of_tiles(24))

    acts = []
    for part in range(2):
        a_moves[part]()

        @pl.loop(0, NTP // GROUP)
        def _(i, part=part):
            pieces = [
                z_buf[part, GROUP * i + g, :, n * 128 : (n + 1) * 128].astype(F32)
                for g in range(GROUP)
                for n in range(FEAT // 128)
            ]
            for n, x in enumerate(quantized_lanes(pieces, a_peak, pick_buf[...])):
                act_all[ss, part, :, pl.ds(pl.multiple_of(i * GROUP * FEAT + n * 128, 128), 128)] = x

        acts.append(
            SeqGather(
                lambda i, part=part: act_all.at[i, part],
                lambda i, h, part=part: act_all.at[i, part, pl.ds(h * (HALF // 2), HALF // 2)],
                act_all.at[pl.ds(0, NSEQ - 1), part],
            )
        )
        progress(13 + 2 * part)

    part_seven = part_buf.at[pl.ds(0, NSEQ - 1)]
    out_send, out_recv = copies.sender(part_seven), copies.receiver()

    def sub_of(i):
        return lax.rem(dd + i + lax.div(i, 2) - 2 * lax.div(i, 3), NDP)

    def project(dy, first, count):
        chip = lax.rem(yy + dy + 4, 4)

        @pl.loop(first, first + count)
        def _(i):
            lhs = act_all[pl.ds(chip * 2, 2)].reshape(2 * OWN, NTP * FEAT)
            prod = jnp.dot(lhs, w_all[sub_of(i)], preferred_element_type=F32).astype(BF16)
            out_buf[chip * 2, i] = prod[:OWN]
            out_buf[chip * 2 + 1, i] = prod[OWN:]

        subs = pl.ds(first, count)
        for dc in range(2):
            to = sid(dy, dc)
            if dy == 0 and dc == 0:
                part_buf[ss, first : first + count] = out_buf[ss, first : first + count]
            else:
                copies.start(out_buf.at[to, subs], part_buf.at[ss, subs], {"seq": to}, out_send, out_recv)

    acts[0].low()
    acts[0].high()
    progress(16)
    acts[1].low()
    acts[1].high()
    progress(17)
    acts[0].far()
    progress(len(events))
    for a in acts:
        a.x0()
    project(0, 0, 3)
    acts[1].far()
    for a in acts:
        a.x3()
    project(-1, 0, 3)
    for a in acts:
        a.x5()
    project(1, 0, 3)
    for a in acts:
        a.x7()
    project(2, 0, 3)
    for j in range(8):
        x_far[j]()
    for dy in (2, -1, 1, 0):
        project(dy, 3, 1)
    loads[8].wait()
    copies.arrived(out_recv, part_seven)

    square = jnp.zeros((OWN, 128), F32)
    for i in range(NSEQ):
        for j in range(NDP):
            cols = pl.ds(pl.multiple_of(i * COLS + sub_of(j) * SUB, SUB), SUB)
            hid = res_buf[:, cols].astype(F32) + part_buf[i, j].astype(F32)
            hid_buf[:, cols] = hid
            sqr = hid * hid
            for n in range(SUB // 128):
                square = square + sqr[:, n * 128 : (n + 1) * 128]
    store = pltpu.make_async_copy(hid_buf, hid_ref, local_sems.at[9])
    store.start()
    mean = jnp.sum(square, axis=1, keepdims=True) * (1.0 / D)
    root = jnp.broadcast_to(lax.rsqrt(mean + 1e-05), (OWN, 128))
    root_buf[...] = root
    store_root = pltpu.make_async_copy(root_buf, root_ref, local_sems.at[10])
    store_root.start()
    top = jnp.zeros((OWN, 128), F32)
    for i in range(D // 128):
        top = jnp.maximum(top, jnp.abs(hid_buf[:, i * 128 : (i + 1) * 128] * root * gain_ref[i : i + 1, :].astype(F32)))
    tiles[51] = jnp.max(top.reshape(OWN // 8, 8, 128), axis=0)
    tiles[32 + tt] = tiles[51]
    spread_tile(51, 32, "tp", zt)()
    tiles[52] = max_of_tiles(32)
    tiles[40 + ss] = tiles[52]
    spread_tile(52, 40, "seq", sq)()
    tiles[53] = max_of_tiles(40)
    store_top = pltpu.make_async_copy(tiles.at[53], top_ref, local_sems.at[11])
    store_top.start()

    assert len(copies.sent) == N_SEND and copies.n_recv == N_RECV
    copies.finish()
    store.wait()
    store_root.wait()
    store_top.wait()


STEPS = 4
TILES = 8


def quantize_kernel(hid_ref, root_ref, gain_ref, top_ref, new_ref, next_ref):
    peak = jnp.max(top_ref[...])
    pick = pick_matrix()
    root = root_ref[...]

    @pl.loop(0, D // STEPS // 128 // TILES)
    def _(i):
        pieces, cols = [], []
        for n in range(TILES):
            cols.append(pl.ds(pl.multiple_of((i * TILES + n) * 128, 128), 128))
            hid = hid_ref[:, cols[n]]
            new_ref[:, cols[n]] = hid.astype(BF16)
            gain = gain_ref[pl.ds(i * TILES + n, 1), :].astype(F32)
            pieces.append(hid * root * gain)
        for n, x in enumerate(quantized_lanes(pieces, peak, pick)):
            next_ref[:, cols[n]] = x


def local(queries, keys, values, out_weight, residual, norm_gain):
    any_space = pl.BlockSpec(memory_space=pl.ANY)
    vmem = pl.BlockSpec(memory_space=pltpu.VMEM)
    gain = norm_gain.reshape(D // 128, 128).astype(F32)
    hid, root, top = pl.pallas_call(
        kernel,
        out_shape=(
            jax.ShapeDtypeStruct((OWN, D), F32),
            jax.ShapeDtypeStruct((OWN, 128), F32),
            jax.ShapeDtypeStruct((8, 128), F32),
        ),
        in_specs=[any_space] * 5 + [vmem],
        out_specs=(any_space, any_space, any_space),
        scratch_shapes=[
            pltpu.VMEM((TOK, FEAT), BF16),
            pltpu.VMEM((NSEQ, 2, TOK, HEAD), BF16),
            pltpu.VMEM((FEAT, D), BF16),
            pltpu.VMEM((FEAT, SUB), BF16),
            pltpu.VMEM((NDP, NTP * FEAT, SUB), BF16),
            pltpu.VMEM((HEAD, TOK), BF16),
            pltpu.VMEM((HEADS, 1, TOK), F32),
            pltpu.VMEM((HEADS, 1, TOK), F32),
            pltpu.VMEM((HEADS, HEAD, TOK), F32),
            pltpu.VMEM((TOK, FEAT), BF16),
            pltpu.VMEM((2, NTP, HALF, FEAT), BF16),
            pltpu.VMEM((NSEQ, 2, HALF, NTP * FEAT), BF16),
            pltpu.VMEM((NSEQ, NDP, OWN, SUB), BF16),
            pltpu.VMEM((NSEQ, NDP, OWN, SUB), BF16),
            pltpu.VMEM((OWN, D), BF16),
            pltpu.VMEM((OWN, D), F32),
            pltpu.VMEM((56, 8, 128), F32),
            pltpu.VMEM((128, 128), BF16),
            pltpu.VMEM((OWN, 128), F32),
            pltpu.SemaphoreType.DMA((N_SEND,)),
            pltpu.SemaphoreType.DMA((N_RECV,)),
            pltpu.SemaphoreType.DMA((12,)),
        ],
        compiler_params=pltpu.CompilerParams(
            collective_id=0, has_side_effects=True, vmem_limit_bytes=60 * 1024 * 1024
        ),
    )(queries, keys, values, out_weight, residual, gain)
    out = jax.ShapeDtypeStruct((OWN, D), BF16)
    wide = pl.BlockSpec((OWN, D // STEPS), lambda i: (0, i))
    return pl.pallas_call(
        quantize_kernel,
        grid=(STEPS,),
        out_shape=(out, out),
        in_specs=[
            wide,
            pl.BlockSpec((OWN, 128), lambda i: (0, 0)),
            pl.BlockSpec((D // STEPS // 128, 128), lambda i: (i, 0)),
            pl.BlockSpec((8, 128), lambda i: (0, 0)),
        ],
        out_specs=(wide, wide),
    )(hid, root, gain, top)


def solution(mesh):
    in_specs = (
        P(("dp", "seq"), "tp"),
        P(("dp", "seq"), "tp"),
        P(("dp", "seq"), "tp"),
        P("tp", None),
        P(("dp", "seq", "tp"), None),
        P(),
    )
    out_specs = (P(("dp", "seq", "tp"), None), P(("dp", "seq", "tp"), None))
    return jax.shard_map(local, mesh=mesh, in_specs=in_specs, out_specs=out_specs, check_vma=False)
```

```python
import jax
import jax.numpy as jnp
from jax import lax
from jax.experimental import pallas as pl
from jax.experimental.pallas import tpu as pltpu
from jax.sharding import PartitionSpec as P

D = 8192
HEAD = 128
FLOOR = 256.0
NEG = -1e30
MESH = pl.DeviceIdType.MESH
F32 = jnp.float32
BF16 = jnp.bfloat16

TOK = 512
HEADS = 4
FEAT = HEADS * HEAD
NTP = 8
NSEQ = 8
NDP = 4
OWN = TOK // NTP
COLS = D // NSEQ
SUB = COLS // NDP
PAIR = 4
HALF = OWN // 2
GROUP = 2
RA = 416
SCALE = HEAD ** (-0.5) * 1.4426950408889634

SINE = (
    -1.7606472969055176,
    5.904375076293945,
    -10.969871520996094,
    11.68786334991455,
    -5.921726226806641,
    0.8999996781349182,
)


def rounded(x, double):
    v = x / double
    f = v - jnp.round(v)
    z = f * f
    sine = SINE[0] * z + SINE[1]
    for co in SINE[2:]:
        sine = sine * z + co
    half = (v - f * sine).astype(BF16).astype(F32)
    return (half * double).astype(BF16)


def quantized_rows(x, peak):
    n, cols = x.shape
    x = x.reshape(n // 16, 16, cols)
    top = jnp.max(jnp.abs(x), axis=1, keepdims=True)
    tensor_scale = peak / (6.0 * 448.0)
    scale = jnp.maximum(top * (1.0 / (6.0 * tensor_scale)), FLOOR).astype(BF16).astype(F32)
    return rounded(x, jnp.broadcast_to(scale * (2.0 * tensor_scale), x.shape)).reshape(n, cols)


def quantized_lanes(pieces, peak, pick):
    rows = pieces[0].shape[0]
    tensor_scale = peak / (6.0 * 448.0)
    inverse = 1.0 / (6.0 * tensor_scale)
    scales = []
    for x in pieces:
        top = jnp.abs(x)
        for sh in (1, 2, 4, 8):
            top = jnp.maximum(top, pltpu.roll(top, sh, 1))
        scales.append(jnp.maximum(top * inverse, FLOOR).astype(BF16))
    spread = jnp.dot(jnp.concatenate(scales, axis=0), pick, preferred_element_type=F32)
    return [
        rounded(x, spread[i * rows : (i + 1) * rows] * (2.0 * tensor_scale)) for i, x in enumerate(pieces)
    ]


def pick_matrix():
    src = lax.broadcasted_iota(jnp.int32, (128, 128), 0)
    dst = lax.broadcasted_iota(jnp.int32, (128, 128), 1)
    same = (src // 16 == dst // 16) & (src % 16 == 15)
    return jnp.where(same, 1.0, 0.0).astype(BF16)


class Copies:
    def __init__(self, send_sems, recv_sems, dev):
        self.send_sems, self.recv_sems, self.dev = send_sems, recv_sems, dev
        self.sent, self.n_recv = [], 0

    def copy(self, src, dst, send, recv, dev):
        return pltpu.make_async_remote_copy(
            src_ref=src,
            dst_ref=dst,
            send_sem=self.send_sems.at[send],
            recv_sem=self.recv_sems.at[recv],
            device_id=dev,
            device_id_type=MESH,
        )

    def sender(self, total):
        self.sent.append(total)
        return len(self.sent) - 1

    def receiver(self):
        self.n_recv += 1
        return self.n_recv - 1

    def start(self, src, dst, dev, send, recv):
        self.copy(src, dst, send, recv, dev).start()

    def start_one(self, src, dst, dev, send, landing):
        recv = self.receiver()
        self.start(src, dst, dev, send, recv)
        return lambda: self.arrived(recv, landing)

    def arrived(self, recv, landing):
        self.copy(landing, landing, 0, recv, self.dev).wait_recv()

    def finish(self):
        for i, total in enumerate(self.sent):
            self.copy(total, total, i, 0, self.dev).wait_send()


N_SEND = 13
N_RECV = 72


def kernel(
    q_hbm,
    k_hbm,
    v_hbm,
    w_hbm,
    res_hbm,
    gain_ref,
    hid_ref,
    root_ref,
    top_ref,
    q_buf,
    kv_buf,
    w_stage,
    w_raw,
    w_all,
    vt_buf,
    m_ref,
    l_ref,
    o_ref,
    att_buf,
    z_buf,
    act_all,
    out_buf,
    part_buf,
    res_buf,
    hid_buf,
    tiles,
    pick_buf,
    root_buf,
    send_sems,
    recv_sems,
    local_sems,
):
    dd, ss, tt = lax.axis_index("dp"), lax.axis_index("seq"), lax.axis_index("tp")
    yy = lax.div(ss, 2)
    cc = ss - 2 * yy

    def sid(dy, dc):
        return lax.rem(yy + dy + 4, 4) * 2 + (cc if dc == 0 else 1 - cc)

    def zt(k):
        return lax.rem(tt + k + 2 * NTP, NTP)

    def sq(k):
        return lax.rem(ss + k + 2 * NSEQ, NSEQ)

    def xd(k):
        return lax.rem(dd + k + 2 * NDP, NDP)

    loads = [
        pltpu.make_async_copy(k_hbm, kv_buf.at[ss, 0], local_sems.at[0]),
        pltpu.make_async_copy(v_hbm, kv_buf.at[ss, 1], local_sems.at[1]),
        pltpu.make_async_copy(q_hbm, q_buf, local_sems.at[2]),
        pltpu.make_async_copy(
            w_hbm.at[:, pl.ds(pl.multiple_of(ss * COLS + dd * SUB, SUB), SUB)],
            w_raw.at[dd],
            local_sems.at[3],
        ),
    ]
    for i in range(4):
        loads.append(
            pltpu.make_async_copy(
                w_hbm.at[pl.ds(i * 128, 128)], w_stage.at[pl.ds(i * 128, 128)], local_sems.at[4 + i]
            )
        )
    loads.append(pltpu.make_async_copy(res_hbm, res_buf, local_sems.at[8]))
    for load in loads:
        load.start()

    barrier = pltpu.get_barrier_semaphore()
    for k in range(1, NTP):
        pl.semaphore_signal(barrier, inc=1, device_id={"tp": zt(k)}, device_id_type=MESH)
    for k in range(1, NSEQ):
        pl.semaphore_signal(barrier, inc=1, device_id={"seq": sq(k)}, device_id_type=MESH)
    for k in (1, 3):
        pl.semaphore_signal(barrier, inc=1, device_id={"dp": xd(k)}, device_id_type=MESH)

    copies = Copies(send_sems, recv_sems, {"tp": zt(1)})
    pick_buf[...] = pick_matrix()

    class SeqGather:
        def __init__(self, unit, half, total):
            self.unit, self.half, self.send = unit, half, copies.sender(total)
            own = unit(sid(0, 0))
            self.x1 = self.go(own, sid(1, 0), unit(sid(-1, 0)))
            self.x2 = self.go(own, sid(-1, 0), unit(sid(1, 0)))
            self.x0 = self.go(own, sid(0, 1), unit(sid(0, 1)))

        def go(self, ref, to, landing):
            return copies.start_one(ref, ref, {"seq": to}, self.send, landing)

        def low(self):
            self.x1()
            got, part = self.unit(sid(-1, 0)), self.half(sid(-1, 0), 0)
            self.x4 = self.go(part, sid(1, 0), self.half(sid(2, 0), 0))
            self.x3 = self.go(got, sid(0, 1), self.unit(sid(-1, 1)))

        def high(self):
            self.x2()
            got, part = self.unit(sid(1, 0)), self.half(sid(1, 0), 1)
            self.x6 = self.go(part, sid(-1, 0), self.half(sid(2, 0), 1))
            self.x5 = self.go(got, sid(0, 1), self.unit(sid(1, 1)))

        def far(self):
            self.x4()
            self.x6()
            self.x7 = self.go(self.unit(sid(2, 0)), sid(0, 1), self.unit(sid(2, 1)))

    def spread_tile(src, dst_of, axis, at):
        me = tt if axis == "tp" else ss
        seven = tiles.at[pl.ds(dst_of, 7)]
        send, recv = copies.sender(seven), copies.receiver()
        for k in range(1, 8):
            copies.start(tiles.at[src], tiles.at[dst_of + me], {axis: at(k)}, send, recv)
        return lambda: copies.arrived(recv, seven)

    def max_of_tiles(first):
        top = tiles[first]
        for i in range(1, 8):
            top = jnp.maximum(top, tiles[first + i])
        return top

    tiles[48] = jnp.zeros((8, 128), F32)
    for i in range(4):
        loads[4 + i].wait()

        @pl.loop(0, 16)
        def _(j, i=i):
            top = tiles[48]
            piece = jnp.abs(w_stage[i * 128 : (i + 1) * 128, pl.ds(pl.multiple_of(j * 512, 512), 512)].astype(F32))
            top4 = jnp.max(piece.reshape(16, 8, 512), axis=0)
            for n in range(4):
                top = jnp.maximum(top, top4[:, n * 128 : (n + 1) * 128])
            tiles[48] = top

    tiles[8 + tt] = tiles[48]
    pl.semaphore_wait(barrier, NTP - 1 + NSEQ - 1 + 2)
    loads[0].wait()
    loads[1].wait()
    kv = SeqGather(lambda i: kv_buf.at[i], lambda i, h: kv_buf.at[i, h], kv_buf.at[pl.ds(0, NSEQ - 1)])

    loads[3].wait()
    raw_send = copies.sender(w_raw.at[pl.ds(0, NDP - 1)])
    raw_far = []

    def raw_go(ref, to, landing):
        return copies.start_one(ref, ref, {"dp": to}, raw_send, landing)

    raw_left = raw_go(w_raw.at[dd], xd(1), w_raw.at[xd(-1)])
    raw_right = raw_go(w_raw.at[dd], xd(-1), w_raw.at[xd(1)])

    def raw_forward():
        for arrival, d, to, rows in (
            (raw_left, xd(-1), xd(1), pl.ds(0, FEAT // 2)),
            (raw_right, xd(1), xd(-1), pl.ds(FEAT // 2, FEAT // 2)),
        ):
            arrival()
            raw_far.append(raw_go(w_raw.at[d, rows], to, w_raw.at[xd(2), rows]))


    w_top = spread_tile(48, 8, "tp", zt)

    def attend(block, kind):
        vt_buf[...] = kv_buf[block, 1].T

        @pl.loop(0, HEADS // PAIR)
        def _(i):
            heads = [i * PAIR + n for n in range(PAIR)]
            scores = [
                lax.dot_general(
                    kv_buf[block, 0],
                    q_buf[:, pl.ds(pl.multiple_of(h * HEAD, HEAD), HEAD)],
                    (((1,), (1,)), ((), ())),
                    preferred_element_type=F32,
                )
                for h in heads
            ]
            for h, sc in zip(heads, scores):
                if kind == "own":
                    key = lax.broadcasted_iota(jnp.int32, (TOK, TOK), 0)
                    query = lax.broadcasted_iota(jnp.int32, (TOK, TOK), 1)
                    sc = jnp.where(key <= query, sc, NEG)
                top = jnp.max(sc, axis=0, keepdims=True)
                if kind != "own":
                    old = m_ref[h]
                    top = jnp.maximum(old, top)
                p = jnp.exp2((sc - top) * SCALE)
                total = jnp.sum(p, axis=0, keepdims=True)
                o = lax.dot_general(
                    vt_buf[...], p.astype(BF16), (((1,), (0,)), ((), ())), preferred_element_type=F32
                )
                if kind != "own":
                    shrink = jnp.exp2((old - top) * SCALE)
                    total = total + l_ref[h] * shrink
                    o = o + o_ref[h] * shrink
                m_ref[h] = top
                l_ref[h] = total
                o_ref[h] = o

    def attend_if_before(block):
        @pl.when(block < ss)
        def _():
            attend(block, "before")

    loads[2].wait()
    attend(ss, "own")

    w_top()
    w_peak = jnp.max(max_of_tiles(8))

    def quantize_weights(d):
        @pl.loop(0, 4)
        def _(i):
            rows = pl.ds(pl.multiple_of(i * 128, 128), 128)
            to = pl.ds(pl.multiple_of(tt * FEAT + i * 128, 128), 128)
            w_all[d, to, :] = quantized_rows(w_raw[d, rows, :].astype(F32), w_peak)

    quantize_weights(dd)

    def unit_a(d, t):
        return w_all.at[d, pl.ds(pl.multiple_of(t * FEAT, 16), RA)]

    def part_a(d, t, low, high):
        return w_all.at[d, pl.ds(pl.multiple_of(t * FEAT + low, 16), high - low)]

    def bundle_b(t):
        return w_all.at[:, pl.ds(pl.multiple_of(t * FEAT + RA, 16), FEAT - RA)]

    rel = (0, -1, 1, -2, 2, -3, 3, -4)
    up = {0: 0, 1: 1, 2: 3, 3: 5, 4: 7}
    down = {0: 0, 1: 2, 2: 4, 3: 6}
    x_left, x_right, x_far, b_up, b_down, a_up, a_down = {}, {}, {}, {}, {}, {}, {}

    w_send = copies.sender(w_all.at[:, pl.ds(0, 28 * FEAT // NDP)])

    def w_go(ref, to, landing):
        return copies.start_one(ref, ref, to, w_send, landing)

    def x_sends(j):
        t_j = zt(rel[j])
        own = unit_a(dd, t_j)
        x_left[j] = w_go(own, {"dp": xd(1)}, unit_a(xd(-1), t_j))
        x_right[j] = w_go(own, {"dp": xd(-1)}, unit_a(xd(1), t_j))

    def a_send_up(step):
        a_up[step + 1] = w_go(unit_a(dd, zt(-step)), {"tp": zt(1)}, unit_a(dd, zt(-step - 1)))

    def a_send_down(step):
        a_down[step + 1] = w_go(unit_a(dd, zt(step)), {"tp": zt(-1)}, unit_a(dd, zt(step + 1)))

    def b_send_up(step):
        b_up[step + 1] = w_go(bundle_b(zt(-step)), {"tp": zt(1)}, bundle_b(zt(-step - 1)))

    def b_send_down(step):
        b_down[step + 1] = w_go(bundle_b(zt(step)), {"tp": zt(-1)}, bundle_b(zt(step + 1)))

    a_send_up(0)
    a_send_down(0)

    def ev_b0():
        for arrival in raw_far:
            arrival()
        quantize_weights(xd(2))
        b_send_up(0)
        b_send_down(0)

    def ev_a(step):
        def go():
            a_up[step]()
            if step < 4:
                a_send_up(step)
            x_sends(up[step])
            if step < 4:
                a_down[step]()
                if step < 3:
                    a_send_down(step)
                x_sends(down[step])

        return go

    def ev_b(step):
        def go():
            b_up[step]()
            if step < 4:
                b_send_up(step)
                b_down[step]()
                if step < 3:
                    b_send_down(step)

        return go

    def ev_x(j):
        def go():
            t_j = zt(rel[j])
            cut = {7: RA // 2}.get(j, RA if j % 2 == 0 else 0)
            x_left[j]()
            x_far[j] = []
            if cut > 0:
                x_far[j].append(w_go(part_a(xd(-1), t_j, 0, cut), {"dp": xd(1)}, part_a(xd(2), t_j, 0, cut)))
            x_right[j]()
            if cut < RA:
                x_far[j].append(w_go(part_a(xd(1), t_j, cut, RA), {"dp": xd(-1)}, part_a(xd(2), t_j, cut, RA)))

        return go

    kv.x0()
    attend_if_before(sid(0, 1))
    kv.low()
    raw_forward()
    attend_if_before(sid(-1, 0))
    kv.high()
    attend_if_before(sid(1, 0))
    kv.x3()
    attend_if_before(sid(-1, 1))
    kv.far()
    ev_a(1)()
    quantize_weights(xd(-1))
    quantize_weights(xd(1))
    kv.x5()
    attend_if_before(sid(1, 1))
    attend_if_before(sid(2, 0))
    kv.x7()
    ev_b0()
    attend_if_before(sid(2, 1))

    tiles[49] = jnp.zeros((8, 128), F32)
    for h in range(HEADS):
        a = (o_ref[h] / l_ref[h]).T.astype(BF16)
        att_buf[:, h * HEAD : (h + 1) * HEAD] = a
        tiles[49] = jnp.maximum(tiles[49], jnp.max(jnp.abs(a.astype(F32)).reshape(TOK // 8, 8, HEAD), axis=0))
    tiles[16 + tt] = tiles[49]
    a_top = spread_tile(49, 16, "tp", zt)
    a_moves = []
    for part in range(2):
        seven = z_buf.at[part, pl.ds(0, NTP - 1)]
        send, recv = copies.sender(seven), copies.receiver()
        for k in range(1, NTP):
            copies.start(
                att_buf.at[pl.ds(pl.multiple_of(zt(k) * OWN + part * HALF, HALF), HALF)],
                z_buf.at[part, tt],
                {"tp": zt(k)},
                send,
                recv,
            )
        a_moves.append(lambda recv=recv, seven=seven: copies.arrived(recv, seven))
        if part == 0:
            ev_a(2)()
        z_buf[part, tt] = att_buf[pl.ds(pl.multiple_of(tt * OWN + part * HALF, HALF), HALF), :]
    ev_x(1)()
    a_top()
    tiles[50] = max_of_tiles(16)
    tiles[24 + ss] = tiles[50]
    s_top = spread_tile(50, 24, "seq", sq)
    ev_x(2)()
    ev_b(1)()
    s_top()
    a_peak = jnp.max(max_of_tiles(24))
    ev_x(3)()

    acts = []
    for part in range(2):
        a_moves[part]()

        @pl.loop(0, NTP // GROUP)
        def _(i, part=part):
            pieces = [
                z_buf[part, GROUP * i + g, :, n * 128 : (n + 1) * 128].astype(F32)
                for g in range(GROUP)
                for n in range(FEAT // 128)
            ]
            for n, x in enumerate(quantized_lanes(pieces, a_peak, pick_buf[...])):
                act_all[ss, part, :, pl.ds(pl.multiple_of(i * GROUP * FEAT + n * 128, 128), 128)] = x

        acts.append(
            SeqGather(
                lambda i, part=part: act_all.at[i, part],
                lambda i, h, part=part: act_all.at[i, part, pl.ds(h * (HALF // 2), HALF // 2)],
                act_all.at[pl.ds(0, NSEQ - 1), part],
            )
        )
        if part == 0:
            ev_a(3)()

    part_seven = part_buf.at[pl.ds(0, NSEQ - 1)]
    out_send, out_recv = copies.sender(part_seven), copies.receiver()

    def sub_of(i):
        return lax.rem(dd + i + lax.div(i, 2) - 2 * lax.div(i, 3), NDP)

    def project(first, count):
        @pl.loop(0, 4 * count)
        def _(n):
            i = first + lax.div(n, 4)
            chip = lax.rem(yy + 2 + n, 4)
            lhs = act_all[pl.ds(chip * 2, 2)].reshape(2 * OWN, NTP * FEAT)
            prod = jnp.dot(lhs, w_all[sub_of(i)], preferred_element_type=F32).astype(BF16)
            out_buf[chip * 2, i] = prod[:OWN]
            out_buf[chip * 2 + 1, i] = prod[OWN:]

        subs = pl.ds(first, count)
        for dy in (2, 1, -1, 0):
            for dc in range(2):
                to = sid(dy, dc)
                if dy == 0 and dc == 0:
                    part_buf[ss, first : first + count] = out_buf[ss, first : first + count]
                else:
                    copies.start(out_buf.at[to, subs], part_buf.at[ss, subs], {"seq": to}, out_send, out_recv)

    acts[0].low()
    acts[0].high()
    ev_b(2)()
    ev_a(4)()
    ev_x(4)()
    acts[1].low()
    acts[1].high()
    ev_x(5)()
    acts[0].far()
    ev_b(3)()
    acts[1].far()
    ev_x(6)()
    ev_b(4)()
    for a in acts:
        for arrival in (a.x0, a.x3, a.x5, a.x7):
            arrival()
    project(0, 1)
    ev_x(7)()
    project(1, 2)
    for arrivals in x_far.values():
        for arrival in arrivals:
            arrival()
    project(3, 1)
    loads[8].wait()
    copies.arrived(out_recv, part_seven)

    square = jnp.zeros((OWN, 128), F32)
    for i in range(NSEQ):
        for j in range(NDP):
            cols = pl.ds(pl.multiple_of(i * COLS + sub_of(j) * SUB, SUB), SUB)
            hid = res_buf[:, cols].astype(F32) + part_buf[i, j].astype(F32)
            hid_buf[:, cols] = hid
            sqr = hid * hid
            for n in range(SUB // 128):
                square = square + sqr[:, n * 128 : (n + 1) * 128]
    store = pltpu.make_async_copy(hid_buf, hid_ref, local_sems.at[9])
    store.start()
    mean = jnp.sum(square, axis=1, keepdims=True) * (1.0 / D)
    root = jnp.broadcast_to(lax.rsqrt(mean + 1e-05), (OWN, 128))
    root_buf[...] = root
    store_root = pltpu.make_async_copy(root_buf, root_ref, local_sems.at[10])
    store_root.start()
    top = jnp.zeros((OWN, 128), F32)
    for i in range(D // 128):
        top = jnp.maximum(top, jnp.abs(hid_buf[:, i * 128 : (i + 1) * 128] * root * gain_ref[i : i + 1, :].astype(F32)))
    tiles[51] = jnp.max(top.reshape(OWN // 8, 8, 128), axis=0)
    tiles[32 + tt] = tiles[51]
    spread_tile(51, 32, "tp", zt)()
    tiles[52] = max_of_tiles(32)
    tiles[40 + ss] = tiles[52]
    spread_tile(52, 40, "seq", sq)()
    tiles[53] = max_of_tiles(40)
    store_top = pltpu.make_async_copy(tiles.at[53], top_ref, local_sems.at[11])
    store_top.start()

    assert len(copies.sent) == N_SEND and copies.n_recv == N_RECV
    copies.finish()
    store.wait()
    store_root.wait()
    store_top.wait()


STEPS = 4
TILES = 8


def quantize_kernel(hid_ref, root_ref, gain_ref, top_ref, new_ref, next_ref, gain_buf):
    gain_buf[...] = gain_ref[...].astype(F32)
    peak = jnp.max(top_ref[...])
    pick = pick_matrix()
    root = root_ref[...]

    @pl.loop(0, D // STEPS // 128 // TILES)
    def _(i):
        pieces, cols = [], []
        for n in range(TILES):
            cols.append(pl.ds(pl.multiple_of((i * TILES + n) * 128, 128), 128))
            hid = hid_ref[:, cols[n]]
            new_ref[:, cols[n]] = hid.astype(BF16)
            gain = gain_buf[pl.ds(i * TILES + n, 1), :]
            pieces.append(hid * root * gain)
        for n, x in enumerate(quantized_lanes(pieces, peak, pick)):
            next_ref[:, cols[n]] = x


def local(queries, keys, values, out_weight, residual, norm_gain):
    any_space = pl.BlockSpec(memory_space=pl.ANY)
    vmem = pl.BlockSpec(memory_space=pltpu.VMEM)
    gain = norm_gain.reshape(D // 128, 128)
    hid, root, top = pl.pallas_call(
        kernel,
        out_shape=(
            jax.ShapeDtypeStruct((OWN, D), F32),
            jax.ShapeDtypeStruct((OWN, 128), F32),
            jax.ShapeDtypeStruct((8, 128), F32),
        ),
        in_specs=[any_space] * 5 + [vmem],
        out_specs=(any_space, any_space, any_space),
        scratch_shapes=[
            pltpu.VMEM((TOK, FEAT), BF16),
            pltpu.VMEM((NSEQ, 2, TOK, HEAD), BF16),
            pltpu.VMEM((FEAT, D), BF16),
            pltpu.VMEM((NDP, FEAT, SUB), BF16),
            pltpu.VMEM((NDP, NTP * FEAT, SUB), BF16),
            pltpu.VMEM((HEAD, TOK), BF16),
            pltpu.VMEM((HEADS, 1, TOK), F32),
            pltpu.VMEM((HEADS, 1, TOK), F32),
            pltpu.VMEM((HEADS, HEAD, TOK), F32),
            pltpu.VMEM((TOK, FEAT), BF16),
            pltpu.VMEM((2, NTP, HALF, FEAT), BF16),
            pltpu.VMEM((NSEQ, 2, HALF, NTP * FEAT), BF16),
            pltpu.VMEM((NSEQ, NDP, OWN, SUB), BF16),
            pltpu.VMEM((NSEQ, NDP, OWN, SUB), BF16),
            pltpu.VMEM((OWN, D), BF16),
            pltpu.VMEM((OWN, D), F32),
            pltpu.VMEM((56, 8, 128), F32),
            pltpu.VMEM((128, 128), BF16),
            pltpu.VMEM((OWN, 128), F32),
            pltpu.SemaphoreType.DMA((N_SEND,)),
            pltpu.SemaphoreType.DMA((N_RECV,)),
            pltpu.SemaphoreType.DMA((12,)),
        ],
        compiler_params=pltpu.CompilerParams(
            collective_id=0, has_side_effects=True, vmem_limit_bytes=60 * 1024 * 1024
        ),
    )(queries, keys, values, out_weight, residual, gain)
    out = jax.ShapeDtypeStruct((OWN, D), BF16)
    wide = pl.BlockSpec((OWN, D // STEPS), lambda i: (0, i))
    return pl.pallas_call(
        quantize_kernel,
        grid=(STEPS,),
        out_shape=(out, out),
        in_specs=[
            wide,
            pl.BlockSpec((OWN, 128), lambda i: (0, 0)),
            pl.BlockSpec((D // STEPS // 128, 128), lambda i: (i, 0)),
            pl.BlockSpec((8, 128), lambda i: (0, 0)),
        ],
        out_specs=(wide, wide),
        scratch_shapes=[pltpu.VMEM((D // STEPS // 128, 128), F32)],
    )(hid, root, gain, top)


def solution(mesh):
    in_specs = (
        P(("dp", "seq"), "tp"),
        P(("dp", "seq"), "tp"),
        P(("dp", "seq"), "tp"),
        P("tp", None),
        P(("dp", "seq", "tp"), None),
        P(),
    )
    out_specs = (P(("dp", "seq", "tp"), None), P(("dp", "seq", "tp"), None))
    return jax.shard_map(local, mesh=mesh, in_specs=in_specs, out_specs=out_specs, check_vma=False)
```

```python
import jax
import jax.numpy as jnp
from jax import lax
from jax.experimental import pallas as pl
from jax.experimental.pallas import tpu as pltpu
from jax.sharding import PartitionSpec as P

D = 8192
HEAD = 128
FLOOR = 256.0
NEG = -1e30
MESH = pl.DeviceIdType.MESH
F32 = jnp.float32
BF16 = jnp.bfloat16

TOK = 512
HEADS = 4
FEAT = HEADS * HEAD
NTP = 8
NSEQ = 8
NDP = 4
OWN = TOK // NTP
COLS = D // NSEQ
SUB = COLS // NDP
PAIR = 4
HALF = OWN // 2
GROUP = 2
RA = 416
SCALE = HEAD ** (-0.5) * 1.4426950408889634

SINE = (
    -1.7606472969055176,
    5.904375076293945,
    -10.969871520996094,
    11.68786334991455,
    -5.921726226806641,
    0.8999996781349182,
)


def rounded(x, double):
    v = x / double
    f = v - jnp.round(v)
    z = f * f
    sine = SINE[0] * z + SINE[1]
    for co in SINE[2:]:
        sine = sine * z + co
    half = (v - f * sine).astype(BF16).astype(F32)
    return (half * double).astype(BF16)


def quantized_rows(x, peak):
    n, cols = x.shape
    x = x.reshape(n // 16, 16, cols)
    top = jnp.max(jnp.abs(x), axis=1, keepdims=True)
    tensor_scale = peak / (6.0 * 448.0)
    scale = jnp.maximum(top * (1.0 / (6.0 * tensor_scale)), FLOOR).astype(BF16).astype(F32)
    return rounded(x, jnp.broadcast_to(scale * (2.0 * tensor_scale), x.shape)).reshape(n, cols)


def quantized_lanes(pieces, peak, pick):
    rows = pieces[0].shape[0]
    tensor_scale = peak / (6.0 * 448.0)
    inverse = 1.0 / (6.0 * tensor_scale)
    scales = []
    for x in pieces:
        top = jnp.abs(x)
        for sh in (1, 2, 4, 8):
            top = jnp.maximum(top, pltpu.roll(top, sh, 1))
        scales.append(jnp.maximum(top * inverse, FLOOR).astype(BF16))
    spread = jnp.dot(jnp.concatenate(scales, axis=0), pick, preferred_element_type=F32)
    return [
        rounded(x, spread[i * rows : (i + 1) * rows] * (2.0 * tensor_scale)) for i, x in enumerate(pieces)
    ]


def pick_matrix():
    src = lax.broadcasted_iota(jnp.int32, (128, 128), 0)
    dst = lax.broadcasted_iota(jnp.int32, (128, 128), 1)
    same = (src // 16 == dst // 16) & (src % 16 == 15)
    return jnp.where(same, 1.0, 0.0).astype(BF16)


class Copies:
    def __init__(self, send_sems, recv_sems, dev):
        self.send_sems, self.recv_sems, self.dev = send_sems, recv_sems, dev
        self.sent, self.n_recv = [], 0

    def copy(self, src, dst, send, recv, dev):
        return pltpu.make_async_remote_copy(
            src_ref=src,
            dst_ref=dst,
            send_sem=self.send_sems.at[send],
            recv_sem=self.recv_sems.at[recv],
            device_id=dev,
            device_id_type=MESH,
        )

    def sender(self, total):
        self.sent.append(total)
        return len(self.sent) - 1

    def receiver(self):
        self.n_recv += 1
        return self.n_recv - 1

    def start(self, src, dst, dev, send, recv):
        self.copy(src, dst, send, recv, dev).start()

    def start_one(self, src, dst, dev, send, landing):
        recv = self.receiver()
        self.start(src, dst, dev, send, recv)
        return lambda: self.arrived(recv, landing)

    def arrived(self, recv, landing):
        self.copy(landing, landing, 0, recv, self.dev).wait_recv()

    def finish(self):
        for i, total in enumerate(self.sent):
            self.copy(total, total, i, 0, self.dev).wait_send()


N_SEND = 13
N_RECV = 74


def kernel(
    q_hbm,
    k_hbm,
    v_hbm,
    w_hbm,
    res_hbm,
    gain_ref,
    hid_ref,
    root_ref,
    top_ref,
    q_buf,
    kv_buf,
    w_stage,
    w_raw,
    w_all,
    vt_buf,
    m_ref,
    l_ref,
    o_ref,
    att_buf,
    z_buf,
    act_all,
    out_buf,
    part_buf,
    res_buf,
    hid_buf,
    tiles,
    pick_buf,
    root_buf,
    send_sems,
    recv_sems,
    local_sems,
):
    dd, ss, tt = lax.axis_index("dp"), lax.axis_index("seq"), lax.axis_index("tp")
    yy = lax.div(ss, 2)
    cc = ss - 2 * yy

    def sid(dy, dc):
        return lax.rem(yy + dy + 4, 4) * 2 + (cc if dc == 0 else 1 - cc)

    def zt(k):
        return lax.rem(tt + k + 2 * NTP, NTP)

    def sq(k):
        return lax.rem(ss + k + 2 * NSEQ, NSEQ)

    def xd(k):
        return lax.rem(dd + k + 2 * NDP, NDP)

    loads = [
        pltpu.make_async_copy(k_hbm, kv_buf.at[ss, 0], local_sems.at[0]),
        pltpu.make_async_copy(v_hbm, kv_buf.at[ss, 1], local_sems.at[1]),
        pltpu.make_async_copy(q_hbm, q_buf, local_sems.at[2]),
        pltpu.make_async_copy(
            w_hbm.at[:, pl.ds(pl.multiple_of(ss * COLS + dd * SUB, SUB), SUB)],
            w_raw.at[dd],
            local_sems.at[3],
        ),
    ]
    for i in range(4):
        loads.append(
            pltpu.make_async_copy(
                w_hbm.at[pl.ds(i * 128, 128)], w_stage.at[pl.ds(i * 128, 128)], local_sems.at[4 + i]
            )
        )
    loads.append(pltpu.make_async_copy(res_hbm, res_buf, local_sems.at[8]))
    for load in loads:
        load.start()

    barrier = pltpu.get_barrier_semaphore()
    for k in range(1, NTP):
        pl.semaphore_signal(barrier, inc=1, device_id={"tp": zt(k)}, device_id_type=MESH)
    for k in range(1, NSEQ):
        pl.semaphore_signal(barrier, inc=1, device_id={"seq": sq(k)}, device_id_type=MESH)
    for k in (1, 3):
        pl.semaphore_signal(barrier, inc=1, device_id={"dp": xd(k)}, device_id_type=MESH)

    copies = Copies(send_sems, recv_sems, {"tp": zt(1)})
    pick_buf[...] = pick_matrix()

    class SeqGather:
        def __init__(self, unit, half, total):
            self.unit, self.half, self.send = unit, half, copies.sender(total)
            own = unit(sid(0, 0))
            self.x1 = self.go(own, sid(1, 0), unit(sid(-1, 0)))
            self.x2 = self.go(own, sid(-1, 0), unit(sid(1, 0)))
            self.x0 = self.go(own, sid(0, 1), unit(sid(0, 1)))

        def go(self, ref, to, landing):
            return copies.start_one(ref, ref, {"seq": to}, self.send, landing)

        def low(self):
            self.x1()
            got, part = self.unit(sid(-1, 0)), self.half(sid(-1, 0), 0)
            self.x4 = self.go(part, sid(1, 0), self.half(sid(2, 0), 0))
            self.x3 = self.go(got, sid(0, 1), self.unit(sid(-1, 1)))

        def high(self):
            self.x2()
            got, part = self.unit(sid(1, 0)), self.half(sid(1, 0), 1)
            self.x6 = self.go(part, sid(-1, 0), self.half(sid(2, 0), 1))
            self.x5 = self.go(got, sid(0, 1), self.unit(sid(1, 1)))

        def far(self):
            self.x4()
            self.x6()
            self.x7 = self.go(self.unit(sid(2, 0)), sid(0, 1), self.unit(sid(2, 1)))

    def spread_tile(src, dst_of, axis, at):
        me = tt if axis == "tp" else ss
        seven = tiles.at[pl.ds(dst_of, 7)]
        send, recv = copies.sender(seven), copies.receiver()
        for k in range(1, 8):
            copies.start(tiles.at[src], tiles.at[dst_of + me], {axis: at(k)}, send, recv)
        return lambda: copies.arrived(recv, seven)

    def max_of_tiles(first):
        top = tiles[first]
        for i in range(1, 8):
            top = jnp.maximum(top, tiles[first + i])
        return top

    tiles[48] = jnp.zeros((8, 128), F32)
    for i in range(4):
        loads[4 + i].wait()

        @pl.loop(0, 16)
        def _(j, i=i):
            top = tiles[48]
            piece = jnp.abs(w_stage[i * 128 : (i + 1) * 128, pl.ds(pl.multiple_of(j * 512, 512), 512)].astype(F32))
            top4 = jnp.max(piece.reshape(16, 8, 512), axis=0)
            for n in range(4):
                top = jnp.maximum(top, top4[:, n * 128 : (n + 1) * 128])
            tiles[48] = top

    tiles[8 + tt] = tiles[48]
    pl.semaphore_wait(barrier, NTP - 1 + NSEQ - 1 + 2)
    loads[0].wait()
    loads[1].wait()
    kv = SeqGather(lambda i: kv_buf.at[i], lambda i, h: kv_buf.at[i, h], kv_buf.at[pl.ds(0, NSEQ - 1)])

    loads[3].wait()
    raw_send = copies.sender(w_raw.at[pl.ds(0, NDP - 1)])
    raw_far = []

    def raw_go(ref, to, landing):
        return copies.start_one(ref, ref, {"dp": to}, raw_send, landing)

    raw_left = raw_go(w_raw.at[dd], xd(1), w_raw.at[xd(-1)])
    raw_right = raw_go(w_raw.at[dd], xd(-1), w_raw.at[xd(1)])

    def raw_forward():
        for arrival, d, to, rows in (
            (raw_left, xd(-1), xd(1), pl.ds(0, FEAT // 2)),
            (raw_right, xd(1), xd(-1), pl.ds(FEAT // 2, FEAT // 2)),
        ):
            arrival()
            raw_far.append(raw_go(w_raw.at[d, rows], to, w_raw.at[xd(2), rows]))


    w_top = spread_tile(48, 8, "tp", zt)

    def attend(block, kind):
        vt_buf[...] = kv_buf[block, 1].T

        @pl.loop(0, HEADS // PAIR)
        def _(i):
            heads = [i * PAIR + n for n in range(PAIR)]
            scores = [
                lax.dot_general(
                    kv_buf[block, 0],
                    q_buf[:, pl.ds(pl.multiple_of(h * HEAD, HEAD), HEAD)],
                    (((1,), (1,)), ((), ())),
                    preferred_element_type=F32,
                )
                for h in heads
            ]
            for h, sc in zip(heads, scores):
                if kind == "own":
                    key = lax.broadcasted_iota(jnp.int32, (TOK, TOK), 0)
                    query = lax.broadcasted_iota(jnp.int32, (TOK, TOK), 1)
                    sc = jnp.where(key <= query, sc, NEG)
                top = jnp.max(sc, axis=0, keepdims=True)
                if kind != "own":
                    old = m_ref[h]
                    top = jnp.maximum(old, top)
                p = jnp.exp2((sc - top) * SCALE)
                total = jnp.sum(p, axis=0, keepdims=True)
                o = lax.dot_general(
                    vt_buf[...], p.astype(BF16), (((1,), (0,)), ((), ())), preferred_element_type=F32
                )
                if kind != "own":
                    shrink = jnp.exp2((old - top) * SCALE)
                    total = total + l_ref[h] * shrink
                    o = o + o_ref[h] * shrink
                m_ref[h] = top
                l_ref[h] = total
                o_ref[h] = o

    def attend_if_before(block):
        @pl.when(block < ss)
        def _():
            attend(block, "before")

    loads[2].wait()
    attend(ss, "own")

    w_top()
    w_peak = jnp.max(max_of_tiles(8))

    def quantize_weights(d):
        @pl.loop(0, 4)
        def _(i):
            rows = pl.ds(pl.multiple_of(i * 128, 128), 128)
            to = pl.ds(pl.multiple_of(tt * FEAT + i * 128, 128), 128)
            w_all[d, to, :] = quantized_rows(w_raw[d, rows, :].astype(F32), w_peak)

    quantize_weights(dd)

    def unit_a(d, t):
        return w_all.at[d, pl.ds(pl.multiple_of(t * FEAT, 16), RA)]

    def part_a(d, t, low, high):
        return w_all.at[d, pl.ds(pl.multiple_of(t * FEAT + low, 16), high - low)]

    def part_b(t, low, high):
        return w_all.at[:, pl.ds(pl.multiple_of(t * FEAT + low, 16), high - low)]

    rel = (0, -1, 1, -2, 2, -3, 3, -4)
    up = {0: 0, 1: 1, 2: 3, 3: 5, 4: 7}
    down = {0: 0, 1: 2, 2: 4, 3: 6}
    x_left, x_right, x_far, b_up, b_down, a_up, a_down = {}, {}, {}, {}, {}, {}, {}

    w_send = copies.sender(w_all.at[:, pl.ds(0, 28 * FEAT // NDP)])

    def w_go(ref, to, landing):
        return copies.start_one(ref, ref, to, w_send, landing)

    def x_sends(j):
        t_j = zt(rel[j])
        own = unit_a(dd, t_j)
        x_left[j] = w_go(own, {"dp": xd(1)}, unit_a(xd(-1), t_j))
        x_right[j] = w_go(own, {"dp": xd(-1)}, unit_a(xd(1), t_j))

    def a_send_up(step):
        cut = RA // 2 if step == 3 else RA
        landing = part_a(dd, zt(-step - 1), 0, cut)
        a_up[step + 1] = w_go(part_a(dd, zt(-step), 0, cut), {"tp": zt(1)}, landing)

    def a_send_down(step):
        cut = RA // 2 if step == 3 else 0
        landing = part_a(dd, zt(step + 1), cut, RA)
        a_down[step + 1] = w_go(part_a(dd, zt(step), cut, RA), {"tp": zt(-1)}, landing)

    def b_send_up(step):
        cut = (RA + FEAT) // 2 if step == 3 else FEAT
        landing = part_b(zt(-step - 1), RA, cut)
        b_up[step + 1] = w_go(part_b(zt(-step), RA, cut), {"tp": zt(1)}, landing)

    def b_send_down(step):
        cut = (RA + FEAT) // 2 if step == 3 else RA
        landing = part_b(zt(step + 1), cut, FEAT)
        b_down[step + 1] = w_go(part_b(zt(step), cut, FEAT), {"tp": zt(-1)}, landing)

    a_send_up(0)
    a_send_down(0)

    def ev_b0():
        for arrival in raw_far:
            arrival()
        quantize_weights(xd(2))
        b_send_up(0)
        b_send_down(0)

    def ev_a(step):
        a_up[step]()
        if step < 4:
            a_send_up(step)
            x_sends(up[step])
        a_down[step]()
        if step < 4:
            a_send_down(step)
            x_sends(down[step])
        else:
            x_sends(up[step])

    def ev_b(step):
        b_up[step]()
        if step < 4:
            b_send_up(step)
        b_down[step]()
        if step < 4:
            b_send_down(step)

    def ev_x(j):
        def go():
            t_j = zt(rel[j])
            cut = {7: RA // 2}.get(j, RA if j % 2 == 0 else 0)
            x_left[j]()
            x_far[j] = []
            if cut > 0:
                x_far[j].append(w_go(part_a(xd(-1), t_j, 0, cut), {"dp": xd(1)}, part_a(xd(2), t_j, 0, cut)))
            x_right[j]()
            if cut < RA:
                x_far[j].append(w_go(part_a(xd(1), t_j, cut, RA), {"dp": xd(-1)}, part_a(xd(2), t_j, cut, RA)))

        return go

    kv.x0()
    attend_if_before(sid(0, 1))
    kv.low()
    kv.high()
    raw_forward()
    attend_if_before(sid(-1, 0))
    attend_if_before(sid(1, 0))
    kv.x3()
    attend_if_before(sid(-1, 1))
    kv.far()
    ev_a(1)
    quantize_weights(xd(-1))
    quantize_weights(xd(1))
    ev_b0()
    kv.x5()
    attend_if_before(sid(1, 1))
    attend_if_before(sid(2, 0))
    kv.x7()
    attend_if_before(sid(2, 1))

    tiles[49] = jnp.zeros((8, 128), F32)
    for h in range(HEADS):
        a = (o_ref[h] / l_ref[h]).T.astype(BF16)
        att_buf[:, h * HEAD : (h + 1) * HEAD] = a
        tiles[49] = jnp.maximum(tiles[49], jnp.max(jnp.abs(a.astype(F32)).reshape(TOK // 8, 8, HEAD), axis=0))
    tiles[16 + tt] = tiles[49]
    a_top = spread_tile(49, 16, "tp", zt)
    a_moves = []
    for part in range(2):
        seven = z_buf.at[part, pl.ds(0, NTP - 1)]
        send, recv = copies.sender(seven), copies.receiver()
        for k in range(1, NTP):
            copies.start(
                att_buf.at[pl.ds(pl.multiple_of(zt(k) * OWN + part * HALF, HALF), HALF)],
                z_buf.at[part, tt],
                {"tp": zt(k)},
                send,
                recv,
            )
        a_moves.append(lambda recv=recv, seven=seven: copies.arrived(recv, seven))
        z_buf[part, tt] = att_buf[pl.ds(pl.multiple_of(tt * OWN + part * HALF, HALF), HALF), :]
    ev_a(2)
    ev_x(1)()
    a_top()
    tiles[50] = max_of_tiles(16)
    tiles[24 + ss] = tiles[50]
    s_top = spread_tile(50, 24, "seq", sq)
    ev_x(2)()
    ev_b(1)
    s_top()
    a_peak = jnp.max(max_of_tiles(24))
    ev_x(3)()

    acts = []
    for part in range(2):
        a_moves[part]()

        @pl.loop(0, NTP // GROUP)
        def _(i, part=part):
            pieces = [
                z_buf[part, GROUP * i + g, :, n * 128 : (n + 1) * 128].astype(F32)
                for g in range(GROUP)
                for n in range(FEAT // 128)
            ]
            for n, x in enumerate(quantized_lanes(pieces, a_peak, pick_buf[...])):
                act_all[ss, part, :, pl.ds(pl.multiple_of(i * GROUP * FEAT + n * 128, 128), 128)] = x

        acts.append(
            SeqGather(
                lambda i, part=part: act_all.at[i, part],
                lambda i, h, part=part: act_all.at[i, part, pl.ds(h * (HALF // 2), HALF // 2)],
                act_all.at[pl.ds(0, NSEQ - 1), part],
            )
        )
        if part == 0:
            ev_x(4)()

    part_seven = part_buf.at[pl.ds(0, NSEQ - 1)]
    out_send, out_recv = copies.sender(part_seven), copies.receiver()

    def sub_of(i):
        return lax.rem(dd + i + lax.div(i, 2) - 2 * lax.div(i, 3), NDP)

    def project(i, low, high):
        @pl.loop(low, high)
        def _(n):
            chip = lax.rem(yy + 1 + 2 * n - lax.div(n, 2), 4)
            lhs = act_all[pl.ds(chip * 2, 2)].reshape(2 * OWN, NTP * FEAT)
            prod = jnp.dot(lhs, w_all[sub_of(i)], preferred_element_type=F32).astype(BF16)
            out_buf[chip * 2, i] = prod[:OWN]
            out_buf[chip * 2 + 1, i] = prod[OWN:]

        for dy in (1, -1, 0, 2)[low:high]:
            for dc in range(2):
                to = sid(dy, dc)
                if dy == 0 and dc == 0:
                    part_buf[ss, i] = out_buf[ss, i]
                else:
                    copies.start(out_buf.at[to, i], part_buf.at[ss, i], {"seq": to}, out_send, out_recv)

    ev_a(3)
    acts[0].low()
    acts[0].high()
    ev_b(2)
    acts[1].low()
    acts[1].high()
    ev_a(4)
    ev_x(5)()
    acts[0].far()
    ev_b(3)
    acts[1].far()
    ev_x(6)()
    ev_b(4)
    for a in acts:
        for arrival in (a.x0, a.x3, a.x5):
            arrival()
    project(0, 0, 3)
    for a in acts:
        a.x7()
    project(0, 3, 4)
    ev_x(7)()
    project(1, 0, 4)
    project(2, 0, 4)
    for arrivals in x_far.values():
        for arrival in arrivals:
            arrival()
    project(3, 0, 4)
    loads[8].wait()
    copies.arrived(out_recv, part_seven)

    square = jnp.zeros((OWN, 128), F32)
    for i in range(NSEQ):
        for j in range(NDP):
            cols = pl.ds(pl.multiple_of(i * COLS + sub_of(j) * SUB, SUB), SUB)
            hid = res_buf[:, cols].astype(F32) + part_buf[i, j].astype(F32)
            hid_buf[:, cols] = hid
            sqr = hid * hid
            for n in range(SUB // 128):
                square = square + sqr[:, n * 128 : (n + 1) * 128]
    store = pltpu.make_async_copy(hid_buf, hid_ref, local_sems.at[9])
    store.start()
    mean = jnp.sum(square, axis=1, keepdims=True) * (1.0 / D)
    root = jnp.broadcast_to(lax.rsqrt(mean + 1e-05), (OWN, 128))
    root_buf[...] = root
    store_root = pltpu.make_async_copy(root_buf, root_ref, local_sems.at[10])
    store_root.start()
    top = jnp.zeros((OWN, 128), F32)
    for i in range(D // 128):
        top = jnp.maximum(top, jnp.abs(hid_buf[:, i * 128 : (i + 1) * 128] * root * gain_ref[i : i + 1, :].astype(F32)))
    tiles[51] = jnp.max(top.reshape(OWN // 8, 8, 128), axis=0)
    tiles[32 + tt] = tiles[51]
    spread_tile(51, 32, "tp", zt)()
    tiles[52] = max_of_tiles(32)
    tiles[40 + ss] = tiles[52]
    spread_tile(52, 40, "seq", sq)()
    tiles[53] = max_of_tiles(40)
    store_top = pltpu.make_async_copy(tiles.at[53], top_ref, local_sems.at[11])
    store_top.start()

    assert len(copies.sent) == N_SEND and copies.n_recv == N_RECV
    copies.finish()
    store.wait()
    store_root.wait()
    store_top.wait()


STEPS = 4
TILES = 8


def quantize_kernel(hid_ref, root_ref, gain_ref, top_ref, new_ref, next_ref, gain_buf):
    gain_buf[...] = gain_ref[...].astype(F32)
    peak = jnp.max(top_ref[...])
    pick = pick_matrix()
    root = root_ref[...]

    @pl.loop(0, D // STEPS // 128 // TILES)
    def _(i):
        pieces, cols = [], []
        for n in range(TILES):
            cols.append(pl.ds(pl.multiple_of((i * TILES + n) * 128, 128), 128))
            hid = hid_ref[:, cols[n]]
            new_ref[:, cols[n]] = hid.astype(BF16)
            gain = gain_buf[pl.ds(i * TILES + n, 1), :]
            pieces.append(hid * root * gain)
        for n, x in enumerate(quantized_lanes(pieces, peak, pick)):
            next_ref[:, cols[n]] = x


def local(queries, keys, values, out_weight, residual, norm_gain):
    any_space = pl.BlockSpec(memory_space=pl.ANY)
    vmem = pl.BlockSpec(memory_space=pltpu.VMEM)
    gain = norm_gain.reshape(D // 128, 128)
    hid, root, top = pl.pallas_call(
        kernel,
        out_shape=(
            jax.ShapeDtypeStruct((OWN, D), F32),
            jax.ShapeDtypeStruct((OWN, 128), F32),
            jax.ShapeDtypeStruct((8, 128), F32),
        ),
        in_specs=[any_space] * 5 + [vmem],
        out_specs=(any_space, any_space, any_space),
        scratch_shapes=[
            pltpu.VMEM((TOK, FEAT), BF16),
            pltpu.VMEM((NSEQ, 2, TOK, HEAD), BF16),
            pltpu.VMEM((FEAT, D), BF16),
            pltpu.VMEM((NDP, FEAT, SUB), BF16),
            pltpu.VMEM((NDP, NTP * FEAT, SUB), BF16),
            pltpu.VMEM((HEAD, TOK), BF16),
            pltpu.VMEM((HEADS, 1, TOK), F32),
            pltpu.VMEM((HEADS, 1, TOK), F32),
            pltpu.VMEM((HEADS, HEAD, TOK), F32),
            pltpu.VMEM((TOK, FEAT), BF16),
            pltpu.VMEM((2, NTP, HALF, FEAT), BF16),
            pltpu.VMEM((NSEQ, 2, HALF, NTP * FEAT), BF16),
            pltpu.VMEM((NSEQ, NDP, OWN, SUB), BF16),
            pltpu.VMEM((NSEQ, NDP, OWN, SUB), BF16),
            pltpu.VMEM((OWN, D), BF16),
            pltpu.VMEM((OWN, D), F32),
            pltpu.VMEM((56, 8, 128), F32),
            pltpu.VMEM((128, 128), BF16),
            pltpu.VMEM((OWN, 128), F32),
            pltpu.SemaphoreType.DMA((N_SEND,)),
            pltpu.SemaphoreType.DMA((N_RECV,)),
            pltpu.SemaphoreType.DMA((12,)),
        ],
        compiler_params=pltpu.CompilerParams(
            collective_id=0, has_side_effects=True, vmem_limit_bytes=60 * 1024 * 1024
        ),
    )(queries, keys, values, out_weight, residual, gain)
    out = jax.ShapeDtypeStruct((OWN, D), BF16)
    wide = pl.BlockSpec((OWN, D // STEPS), lambda i: (0, i))
    return pl.pallas_call(
        quantize_kernel,
        grid=(STEPS,),
        out_shape=(out, out),
        in_specs=[
            wide,
            pl.BlockSpec((OWN, 128), lambda i: (0, 0)),
            pl.BlockSpec((D // STEPS // 128, 128), lambda i: (i, 0)),
            pl.BlockSpec((8, 128), lambda i: (0, 0)),
        ],
        out_specs=(wide, wide),
        scratch_shapes=[pltpu.VMEM((D // STEPS // 128, 128), F32)],
    )(hid, root, gain, top)


def solution(mesh):
    in_specs = (
        P(("dp", "seq"), "tp"),
        P(("dp", "seq"), "tp"),
        P(("dp", "seq"), "tp"),
        P("tp", None),
        P(("dp", "seq", "tp"), None),
        P(),
    )
    out_specs = (P(("dp", "seq", "tp"), None), P(("dp", "seq", "tp"), None))
    return jax.shard_map(local, mesh=mesh, in_specs=in_specs, out_specs=out_specs, check_vma=False)
```

```python
import jax
import jax.numpy as jnp
from jax import lax
from jax.experimental import pallas as pl
from jax.experimental.pallas import tpu as pltpu
from jax.sharding import PartitionSpec as P

D = 8192
HEAD = 128
FLOOR = 256.0
NEG = -1e30
MESH = pl.DeviceIdType.MESH
F32 = jnp.float32
BF16 = jnp.bfloat16

TOK = 512
HEADS = 4
FEAT = HEADS * HEAD
NTP = 8
NSEQ = 8
NDP = 4
OWN = TOK // NTP
COLS = D // NSEQ
SUB = COLS // NDP
PAIR = 4
HALF = OWN // 2
GROUP = 2
RA = 416
SCALE = HEAD ** (-0.5) * 1.4426950408889634

SINE = (
    -1.7606472969055176,
    5.904375076293945,
    -10.969871520996094,
    11.68786334991455,
    -5.921726226806641,
    0.8999996781349182,
)


def rounded(x, double):
    v = x / double
    f = v - jnp.round(v)
    z = f * f
    sine = SINE[0] * z + SINE[1]
    for co in SINE[2:]:
        sine = sine * z + co
    half = (v - f * sine).astype(BF16).astype(F32)
    return (half * double).astype(BF16)


def quantized_rows(x, peak):
    n, cols = x.shape
    x = x.reshape(n // 16, 16, cols)
    top = jnp.max(jnp.abs(x), axis=1, keepdims=True)
    tensor_scale = peak / (6.0 * 448.0)
    scale = jnp.maximum(top * (1.0 / (6.0 * tensor_scale)), FLOOR).astype(BF16).astype(F32)
    return rounded(x, jnp.broadcast_to(scale * (2.0 * tensor_scale), x.shape)).reshape(n, cols)


def lane_tops(x):
    top = jnp.abs(x)
    for sh in (1, 2, 4, 8):
        top = jnp.maximum(top, pltpu.roll(top, sh, 1))
    return top


def quantized_lanes(pieces, tops, peak, pick):
    rows = pieces[0].shape[0]
    tensor_scale = peak / (6.0 * 448.0)
    inverse = 1.0 / (6.0 * tensor_scale)
    scales = [jnp.maximum(top * inverse, FLOOR).astype(BF16) for top in tops]
    spread = jnp.dot(jnp.concatenate(scales, axis=0), pick, preferred_element_type=F32)
    return [
        rounded(x, spread[i * rows : (i + 1) * rows] * (2.0 * tensor_scale)) for i, x in enumerate(pieces)
    ]


def pick_matrix():
    src = lax.broadcasted_iota(jnp.int32, (128, 128), 0)
    dst = lax.broadcasted_iota(jnp.int32, (128, 128), 1)
    same = (src // 16 == dst // 16) & (src % 16 == 15)
    return jnp.where(same, 1.0, 0.0).astype(BF16)


class Copies:
    def __init__(self, send_sems, recv_sems, dev):
        self.send_sems, self.recv_sems, self.dev = send_sems, recv_sems, dev
        self.sent, self.n_recv = [], 0

    def copy(self, src, dst, send, recv, dev):
        return pltpu.make_async_remote_copy(
            src_ref=src,
            dst_ref=dst,
            send_sem=self.send_sems.at[send],
            recv_sem=self.recv_sems.at[recv],
            device_id=dev,
            device_id_type=MESH,
        )

    def sender(self, total):
        self.sent.append(total)
        return len(self.sent) - 1

    def receiver(self):
        self.n_recv += 1
        return self.n_recv - 1

    def start(self, src, dst, dev, send, recv):
        self.copy(src, dst, send, recv, dev).start()

    def start_one(self, src, dst, dev, send, landing):
        recv = self.receiver()
        self.start(src, dst, dev, send, recv)
        return lambda: self.arrived(recv, landing)

    def arrived(self, recv, landing):
        self.copy(landing, landing, 0, recv, self.dev).wait_recv()

    def finish(self):
        for i, total in enumerate(self.sent):
            self.copy(total, total, i, 0, self.dev).wait_send()


N_SEND = 13
N_RECV = 74


def kernel(
    q_hbm,
    k_hbm,
    v_hbm,
    w_hbm,
    res_hbm,
    gain_ref,
    hid_ref,
    tops_ref,
    new_ref,
    top_ref,
    q_buf,
    kv_buf,
    w_stage,
    w_raw,
    w_all,
    vt_buf,
    m_ref,
    l_ref,
    o_ref,
    att_buf,
    z_buf,
    act_all,
    out_buf,
    part_buf,
    res_buf,
    hid_buf,
    tiles,
    pick_buf,
    tops_buf,
    new_buf,
    send_sems,
    recv_sems,
    local_sems,
):
    dd, ss, tt = lax.axis_index("dp"), lax.axis_index("seq"), lax.axis_index("tp")
    yy = lax.div(ss, 2)
    cc = ss - 2 * yy

    def sid(dy, dc):
        return lax.rem(yy + dy + 4, 4) * 2 + (cc if dc == 0 else 1 - cc)

    def zt(k):
        return lax.rem(tt + k + 2 * NTP, NTP)

    def sq(k):
        return lax.rem(ss + k + 2 * NSEQ, NSEQ)

    def xd(k):
        return lax.rem(dd + k + 2 * NDP, NDP)

    loads = [
        pltpu.make_async_copy(k_hbm, kv_buf.at[ss, 0], local_sems.at[0]),
        pltpu.make_async_copy(v_hbm, kv_buf.at[ss, 1], local_sems.at[1]),
        pltpu.make_async_copy(q_hbm, q_buf, local_sems.at[2]),
        pltpu.make_async_copy(
            w_hbm.at[:, pl.ds(pl.multiple_of(ss * COLS + dd * SUB, SUB), SUB)],
            w_raw.at[dd],
            local_sems.at[3],
        ),
    ]
    for i in range(4):
        loads.append(
            pltpu.make_async_copy(
                w_hbm.at[pl.ds(i * 128, 128)], w_stage.at[pl.ds(i * 128, 128)], local_sems.at[4 + i]
            )
        )
    loads.append(pltpu.make_async_copy(res_hbm, res_buf, local_sems.at[8]))
    for load in loads:
        load.start()

    barrier = pltpu.get_barrier_semaphore()
    for k in range(1, NTP):
        pl.semaphore_signal(barrier, inc=1, device_id={"tp": zt(k)}, device_id_type=MESH)
    for k in range(1, NSEQ):
        pl.semaphore_signal(barrier, inc=1, device_id={"seq": sq(k)}, device_id_type=MESH)
    for k in (1, 3):
        pl.semaphore_signal(barrier, inc=1, device_id={"dp": xd(k)}, device_id_type=MESH)

    copies = Copies(send_sems, recv_sems, {"tp": zt(1)})
    pick_buf[...] = pick_matrix()

    class SeqGather:
        def __init__(self, unit, half, total):
            self.unit, self.half, self.send = unit, half, copies.sender(total)
            own = unit(sid(0, 0))
            self.x1 = self.go(own, sid(1, 0), unit(sid(-1, 0)))
            self.x2 = self.go(own, sid(-1, 0), unit(sid(1, 0)))
            self.x0 = self.go(own, sid(0, 1), unit(sid(0, 1)))

        def go(self, ref, to, landing):
            return copies.start_one(ref, ref, {"seq": to}, self.send, landing)

        def low(self):
            self.x1()
            got, part = self.unit(sid(-1, 0)), self.half(sid(-1, 0), 0)
            self.x4 = self.go(part, sid(1, 0), self.half(sid(2, 0), 0))
            self.x3 = self.go(got, sid(0, 1), self.unit(sid(-1, 1)))

        def high(self):
            self.x2()
            got, part = self.unit(sid(1, 0)), self.half(sid(1, 0), 1)
            self.x6 = self.go(part, sid(-1, 0), self.half(sid(2, 0), 1))
            self.x5 = self.go(got, sid(0, 1), self.unit(sid(1, 1)))

        def far(self):
            self.x4()
            self.x6()
            self.x7 = self.go(self.unit(sid(2, 0)), sid(0, 1), self.unit(sid(2, 1)))

    def spread_tile(src, dst_of, axis, at):
        me = tt if axis == "tp" else ss
        seven = tiles.at[pl.ds(dst_of, 7)]
        send, recv = copies.sender(seven), copies.receiver()
        for k in range(1, 8):
            copies.start(tiles.at[src], tiles.at[dst_of + me], {axis: at(k)}, send, recv)
        return lambda: copies.arrived(recv, seven)

    def max_of_tiles(first):
        top = tiles[first]
        for i in range(1, 8):
            top = jnp.maximum(top, tiles[first + i])
        return top

    tiles[48] = jnp.zeros((8, 128), F32)
    for i in range(4):
        loads[4 + i].wait()

        @pl.loop(0, 16)
        def _(j, i=i):
            top = tiles[48]
            piece = jnp.abs(w_stage[i * 128 : (i + 1) * 128, pl.ds(pl.multiple_of(j * 512, 512), 512)].astype(F32))
            top4 = jnp.max(piece.reshape(16, 8, 512), axis=0)
            for n in range(4):
                top = jnp.maximum(top, top4[:, n * 128 : (n + 1) * 128])
            tiles[48] = top

    tiles[8 + tt] = tiles[48]
    pl.semaphore_wait(barrier, NTP - 1 + NSEQ - 1 + 2)
    loads[0].wait()
    loads[1].wait()
    kv = SeqGather(lambda i: kv_buf.at[i], lambda i, h: kv_buf.at[i, h], kv_buf.at[pl.ds(0, NSEQ - 1)])

    loads[3].wait()
    raw_send = copies.sender(w_raw.at[pl.ds(0, NDP - 1)])
    raw_far = []

    def raw_go(ref, to, landing):
        return copies.start_one(ref, ref, {"dp": to}, raw_send, landing)

    raw_left = raw_go(w_raw.at[dd], xd(1), w_raw.at[xd(-1)])
    raw_right = raw_go(w_raw.at[dd], xd(-1), w_raw.at[xd(1)])

    def raw_forward():
        for arrival, d, to, rows in (
            (raw_left, xd(-1), xd(1), pl.ds(0, FEAT // 2)),
            (raw_right, xd(1), xd(-1), pl.ds(FEAT // 2, FEAT // 2)),
        ):
            arrival()
            raw_far.append(raw_go(w_raw.at[d, rows], to, w_raw.at[xd(2), rows]))


    w_top = spread_tile(48, 8, "tp", zt)

    def attend(block, kind):
        vt_buf[...] = kv_buf[block, 1].T

        @pl.loop(0, HEADS // PAIR)
        def _(i):
            heads = [i * PAIR + n for n in range(PAIR)]
            scores = [
                lax.dot_general(
                    kv_buf[block, 0],
                    q_buf[:, pl.ds(pl.multiple_of(h * HEAD, HEAD), HEAD)],
                    (((1,), (1,)), ((), ())),
                    preferred_element_type=F32,
                )
                for h in heads
            ]
            for h, sc in zip(heads, scores):
                if kind == "own":
                    key = lax.broadcasted_iota(jnp.int32, (TOK, TOK), 0)
                    query = lax.broadcasted_iota(jnp.int32, (TOK, TOK), 1)
                    sc = jnp.where(key <= query, sc, NEG)
                top = jnp.max(sc, axis=0, keepdims=True)
                if kind != "own":
                    old = m_ref[h]
                    top = jnp.maximum(old, top)
                p = jnp.exp2((sc - top) * SCALE)
                total = jnp.sum(p, axis=0, keepdims=True)
                o = lax.dot_general(
                    vt_buf[...], p.astype(BF16), (((1,), (0,)), ((), ())), preferred_element_type=F32
                )
                if kind != "own":
                    shrink = jnp.exp2((old - top) * SCALE)
                    total = total + l_ref[h] * shrink
                    o = o + o_ref[h] * shrink
                m_ref[h] = top
                l_ref[h] = total
                o_ref[h] = o

    def attend_if_before(block):
        @pl.when(block < ss)
        def _():
            attend(block, "before")

    loads[2].wait()
    attend(ss, "own")

    w_top()
    w_peak = jnp.max(max_of_tiles(8))

    def quantize_weights(d):
        @pl.loop(0, 4)
        def _(i):
            rows = pl.ds(pl.multiple_of(i * 128, 128), 128)
            to = pl.ds(pl.multiple_of(tt * FEAT + i * 128, 128), 128)
            w_all[d, to, :] = quantized_rows(w_raw[d, rows, :].astype(F32), w_peak)

    quantize_weights(dd)

    def unit_a(d, t):
        return w_all.at[d, pl.ds(pl.multiple_of(t * FEAT, 16), RA)]

    def part_a(d, t, low, high):
        return w_all.at[d, pl.ds(pl.multiple_of(t * FEAT + low, 16), high - low)]

    def part_b(t, low, high):
        return w_all.at[:, pl.ds(pl.multiple_of(t * FEAT + low, 16), high - low)]

    rel = (0, -1, 1, -2, 2, -3, 3, -4)
    up = {0: 0, 1: 1, 2: 3, 3: 5, 4: 7}
    down = {0: 0, 1: 2, 2: 4, 3: 6}
    x_left, x_right, x_far, b_up, b_down, a_up, a_down = {}, {}, {}, {}, {}, {}, {}

    w_send = copies.sender(w_all.at[:, pl.ds(0, 28 * FEAT // NDP)])

    def w_go(ref, to, landing):
        return copies.start_one(ref, ref, to, w_send, landing)

    def x_sends(j):
        t_j = zt(rel[j])
        own = unit_a(dd, t_j)
        x_left[j] = w_go(own, {"dp": xd(1)}, unit_a(xd(-1), t_j))
        x_right[j] = w_go(own, {"dp": xd(-1)}, unit_a(xd(1), t_j))

    def a_send_up(step):
        cut = RA // 2 if step == 3 else RA
        landing = part_a(dd, zt(-step - 1), 0, cut)
        a_up[step + 1] = w_go(part_a(dd, zt(-step), 0, cut), {"tp": zt(1)}, landing)

    def a_send_down(step):
        cut = RA // 2 if step == 3 else 0
        landing = part_a(dd, zt(step + 1), cut, RA)
        a_down[step + 1] = w_go(part_a(dd, zt(step), cut, RA), {"tp": zt(-1)}, landing)

    def b_send_up(step):
        cut = (RA + FEAT) // 2 if step == 3 else FEAT
        landing = part_b(zt(-step - 1), RA, cut)
        b_up[step + 1] = w_go(part_b(zt(-step), RA, cut), {"tp": zt(1)}, landing)

    def b_send_down(step):
        cut = (RA + FEAT) // 2 if step == 3 else RA
        landing = part_b(zt(step + 1), cut, FEAT)
        b_down[step + 1] = w_go(part_b(zt(step), cut, FEAT), {"tp": zt(-1)}, landing)

    a_send_up(0)
    a_send_down(0)

    def ev_b0():
        for arrival in raw_far:
            arrival()
        quantize_weights(xd(2))
        b_send_up(0)
        b_send_down(0)

    def ev_a(step):
        a_up[step]()
        if step < 4:
            a_send_up(step)
            x_sends(up[step])
        a_down[step]()
        if step < 4:
            a_send_down(step)
            x_sends(down[step])
        else:
            x_sends(up[step])

    def ev_b(step):
        b_up[step]()
        if step < 4:
            b_send_up(step)
        b_down[step]()
        if step < 4:
            b_send_down(step)

    def ev_x(j):
        def go():
            t_j = zt(rel[j])
            cut = {7: RA // 2}.get(j, RA if j % 2 == 0 else 0)
            x_left[j]()
            x_far[j] = []
            if cut > 0:
                x_far[j].append(w_go(part_a(xd(-1), t_j, 0, cut), {"dp": xd(1)}, part_a(xd(2), t_j, 0, cut)))
            x_right[j]()
            if cut < RA:
                x_far[j].append(w_go(part_a(xd(1), t_j, cut, RA), {"dp": xd(-1)}, part_a(xd(2), t_j, cut, RA)))

        return go

    kv.x0()
    attend_if_before(sid(0, 1))
    kv.low()
    kv.high()
    raw_forward()
    attend_if_before(sid(-1, 0))
    attend_if_before(sid(1, 0))
    kv.x3()
    attend_if_before(sid(-1, 1))
    kv.far()
    ev_a(1)
    quantize_weights(xd(-1))
    quantize_weights(xd(1))
    ev_b0()
    kv.x5()
    attend_if_before(sid(1, 1))
    attend_if_before(sid(2, 0))
    kv.x7()
    attend_if_before(sid(2, 1))

    tiles[49] = jnp.zeros((8, 128), F32)
    for h in range(HEADS):
        a = (o_ref[h] / l_ref[h]).T.astype(BF16)
        att_buf[:, h * HEAD : (h + 1) * HEAD] = a
        tiles[49] = jnp.maximum(tiles[49], jnp.max(jnp.abs(a.astype(F32)).reshape(TOK // 8, 8, HEAD), axis=0))
    tiles[16 + tt] = tiles[49]
    a_top = spread_tile(49, 16, "tp", zt)
    a_moves = []
    for part in range(2):
        seven = z_buf.at[part, pl.ds(0, NTP - 1)]
        send, recv = copies.sender(seven), copies.receiver()
        for k in range(1, NTP):
            copies.start(
                att_buf.at[pl.ds(pl.multiple_of(zt(k) * OWN + part * HALF, HALF), HALF)],
                z_buf.at[part, tt],
                {"tp": zt(k)},
                send,
                recv,
            )
        a_moves.append(lambda recv=recv, seven=seven: copies.arrived(recv, seven))
        z_buf[part, tt] = att_buf[pl.ds(pl.multiple_of(tt * OWN + part * HALF, HALF), HALF), :]
    ev_a(2)
    ev_x(1)()
    a_top()
    tiles[50] = max_of_tiles(16)
    tiles[24 + ss] = tiles[50]
    s_top = spread_tile(50, 24, "seq", sq)
    ev_x(2)()
    ev_b(1)
    s_top()
    a_peak = jnp.max(max_of_tiles(24))
    ev_x(3)()

    acts = []
    for part in range(2):
        a_moves[part]()

        @pl.loop(0, NTP // GROUP)
        def _(i, part=part):
            pieces = [
                z_buf[part, GROUP * i + g, :, n * 128 : (n + 1) * 128].astype(F32)
                for g in range(GROUP)
                for n in range(FEAT // 128)
            ]
            tops = [lane_tops(x) for x in pieces]
            for n, x in enumerate(quantized_lanes(pieces, tops, a_peak, pick_buf[...])):
                act_all[ss, part, :, pl.ds(pl.multiple_of(i * GROUP * FEAT + n * 128, 128), 128)] = x

        acts.append(
            SeqGather(
                lambda i, part=part: act_all.at[i, part],
                lambda i, h, part=part: act_all.at[i, part, pl.ds(h * (HALF // 2), HALF // 2)],
                act_all.at[pl.ds(0, NSEQ - 1), part],
            )
        )
        if part == 0:
            ev_x(4)()

    part_seven = part_buf.at[pl.ds(0, NSEQ - 1)]
    out_send, out_recv = copies.sender(part_seven), copies.receiver()

    def sub_of(i):
        return lax.rem(dd + i + lax.div(i, 2) - 2 * lax.div(i, 3), NDP)

    def project(i, low, high):
        @pl.loop(low, high)
        def _(n):
            chip = lax.rem(yy + 1 + 2 * n - lax.div(n, 2), 4)
            lhs = act_all[pl.ds(chip * 2, 2)].reshape(2 * OWN, NTP * FEAT)
            prod = jnp.dot(lhs, w_all[sub_of(i)], preferred_element_type=F32).astype(BF16)
            out_buf[chip * 2, i] = prod[:OWN]
            out_buf[chip * 2 + 1, i] = prod[OWN:]

        for dy in (1, -1, 0, 2)[low:high]:
            for dc in range(2):
                to = sid(dy, dc)
                if dy == 0 and dc == 0:
                    part_buf[ss, i] = out_buf[ss, i]
                else:
                    copies.start(out_buf.at[to, i], part_buf.at[ss, i], {"seq": to}, out_send, out_recv)

    ev_a(3)
    acts[0].low()
    acts[0].high()
    ev_b(2)
    acts[1].low()
    acts[1].high()
    ev_a(4)
    ev_x(5)()
    acts[0].far()
    ev_b(3)
    acts[1].far()
    ev_x(6)()
    ev_b(4)
    for a in acts:
        for arrival in (a.x0, a.x3, a.x5):
            arrival()
    project(0, 0, 3)
    for a in acts:
        a.x7()
    project(0, 3, 4)
    ev_x(7)()
    project(1, 0, 4)
    project(2, 0, 4)
    for arrivals in x_far.values():
        for arrival in arrivals:
            arrival()
    project(3, 0, 4)
    loads[8].wait()
    copies.arrived(out_recv, part_seven)

    square = jnp.zeros((OWN, 128), F32)
    for i in range(NSEQ):
        for j in range(NDP):
            cols = pl.ds(pl.multiple_of(i * COLS + sub_of(j) * SUB, SUB), SUB)
            hid = res_buf[:, cols].astype(F32) + part_buf[i, j].astype(F32)
            hid_buf[:, cols] = hid
            new_buf[:, cols] = hid.astype(BF16)
            sqr = hid * hid
            for n in range(SUB // 128):
                square = square + sqr[:, n * 128 : (n + 1) * 128]
    stores = [pltpu.make_async_copy(new_buf, new_ref, local_sems.at[9])]
    stores[0].start()
    mean = jnp.sum(square, axis=1, keepdims=True) * (1.0 / D)
    root = lax.rsqrt(mean + 1e-05)
    top = jnp.zeros((OWN, 128), F32)
    for i in range(D // 128):
        cols = slice(i * 128, (i + 1) * 128)
        normed = hid_buf[:, cols] * root * gain_ref[i : i + 1, :].astype(F32)
        hid_buf[:, cols] = normed
        top = jnp.maximum(top, jnp.abs(normed))
    tiles[51] = jnp.max(top.reshape(OWN // 8, 8, 128), axis=0)
    tiles[32 + tt] = tiles[51]
    n_top = spread_tile(51, 32, "tp", zt)
    stores.append(pltpu.make_async_copy(hid_buf, hid_ref, local_sems.at[10]))
    stores[1].start()

    @pl.loop(0, D // 128 // TILES)
    def _(i):
        for n in range(TILES):
            cols = pl.ds(pl.multiple_of((i * TILES + n) * 128, 128), 128)
            tops_buf[:, cols] = lane_tops(hid_buf[:, cols])

    stores.append(pltpu.make_async_copy(tops_buf, tops_ref, local_sems.at[11]))
    stores[2].start()
    n_top()
    tiles[52] = max_of_tiles(32)
    tiles[40 + ss] = tiles[52]
    spread_tile(52, 40, "seq", sq)()
    tiles[53] = max_of_tiles(40)
    stores.append(pltpu.make_async_copy(tiles.at[53], top_ref, local_sems.at[12]))
    stores[3].start()

    assert len(copies.sent) == N_SEND and copies.n_recv == N_RECV
    copies.finish()
    for store in stores:
        store.wait()


STEPS = 4
TILES = 8


def quantize_kernel(hid_ref, tops_ref, sum_ref, top_ref, new_ref, next_ref):
    peak = jnp.max(top_ref[...])
    pick = pick_matrix()

    @pl.loop(0, D // STEPS // 128 // TILES)
    def _(i):
        cols = [pl.ds(pl.multiple_of((i * TILES + n) * 128, 128), 128) for n in range(TILES)]
        pieces = [hid_ref[:, c] for c in cols]
        tops = [tops_ref[:, c] for c in cols]
        for c, x in zip(cols, quantized_lanes(pieces, tops, peak, pick)):
            next_ref[:, c] = x
            new_ref[:, c] = sum_ref[:, c]


def local(queries, keys, values, out_weight, residual, norm_gain):
    any_space = pl.BlockSpec(memory_space=pl.ANY)
    vmem = pl.BlockSpec(memory_space=pltpu.VMEM)
    gain = norm_gain.reshape(D // 128, 128)
    hid, tops, new, top = pl.pallas_call(
        kernel,
        out_shape=(
            jax.ShapeDtypeStruct((OWN, D), F32),
            jax.ShapeDtypeStruct((OWN, D), F32),
            jax.ShapeDtypeStruct((OWN, D), BF16),
            jax.ShapeDtypeStruct((8, 128), F32),
        ),
        in_specs=[any_space] * 5 + [vmem],
        out_specs=(any_space,) * 4,
        scratch_shapes=[
            pltpu.VMEM((TOK, FEAT), BF16),
            pltpu.VMEM((NSEQ, 2, TOK, HEAD), BF16),
            pltpu.VMEM((FEAT, D), BF16),
            pltpu.VMEM((NDP, FEAT, SUB), BF16),
            pltpu.VMEM((NDP, NTP * FEAT, SUB), BF16),
            pltpu.VMEM((HEAD, TOK), BF16),
            pltpu.VMEM((HEADS, 1, TOK), F32),
            pltpu.VMEM((HEADS, 1, TOK), F32),
            pltpu.VMEM((HEADS, HEAD, TOK), F32),
            pltpu.VMEM((TOK, FEAT), BF16),
            pltpu.VMEM((2, NTP, HALF, FEAT), BF16),
            pltpu.VMEM((NSEQ, 2, HALF, NTP * FEAT), BF16),
            pltpu.VMEM((NSEQ, NDP, OWN, SUB), BF16),
            pltpu.VMEM((NSEQ, NDP, OWN, SUB), BF16),
            pltpu.VMEM((OWN, D), BF16),
            pltpu.VMEM((OWN, D), F32),
            pltpu.VMEM((56, 8, 128), F32),
            pltpu.VMEM((128, 128), BF16),
            pltpu.VMEM((OWN, D), F32),
            pltpu.VMEM((OWN, D), BF16),
            pltpu.SemaphoreType.DMA((N_SEND,)),
            pltpu.SemaphoreType.DMA((N_RECV,)),
            pltpu.SemaphoreType.DMA((13,)),
        ],
        compiler_params=pltpu.CompilerParams(
            collective_id=0, has_side_effects=True, vmem_limit_bytes=60 * 1024 * 1024
        ),
    )(queries, keys, values, out_weight, residual, gain)
    out = jax.ShapeDtypeStruct((OWN, D), BF16)
    wide = pl.BlockSpec((OWN, D // STEPS), lambda i: (0, i))
    return pl.pallas_call(
        quantize_kernel,
        grid=(STEPS,),
        out_shape=(out, out),
        in_specs=[wide, wide, wide, pl.BlockSpec((8, 128), lambda i: (0, 0))],
        out_specs=(wide, wide),
    )(hid, tops, new, top)


def solution(mesh):
    in_specs = (
        P(("dp", "seq"), "tp"),
        P(("dp", "seq"), "tp"),
        P(("dp", "seq"), "tp"),
        P("tp", None),
        P(("dp", "seq", "tp"), None),
        P(),
    )
    out_specs = (P(("dp", "seq", "tp"), None), P(("dp", "seq", "tp"), None))
    return jax.shard_map(local, mesh=mesh, in_specs=in_specs, out_specs=out_specs, check_vma=False)
```

```python
import jax
import jax.numpy as jnp
from jax import lax
from jax.experimental import pallas as pl
from jax.experimental.pallas import tpu as pltpu
from jax.sharding import PartitionSpec as P

D = 8192
HEAD = 128
FLOOR = 256.0
NEG = -1e30
MESH = pl.DeviceIdType.MESH
F32 = jnp.float32
BF16 = jnp.bfloat16

TOK = 512
HEADS = 4
FEAT = HEADS * HEAD
NTP = 8
NSEQ = 8
NDP = 4
OWN = TOK // NTP
COLS = D // NSEQ
SUB = COLS // NDP
PAIR = 4
HALF = OWN // 2
GROUP = 2
RA = 416
SCALE = HEAD ** (-0.5) * 1.4426950408889634

SINE = (
    -1.7606472969055176,
    5.904375076293945,
    -10.969871520996094,
    11.68786334991455,
    -5.921726226806641,
    0.8999996781349182,
)


def rounded(x, double):
    v = x / double
    f = v - jnp.round(v)
    z = f * f
    sine = SINE[0] * z + SINE[1]
    for co in SINE[2:]:
        sine = sine * z + co
    half = (v - f * sine).astype(BF16).astype(F32)
    return (half * double).astype(BF16)


def quantized_rows(x, peak):
    n, cols = x.shape
    x = x.reshape(n // 16, 16, cols)
    top = jnp.max(jnp.abs(x), axis=1, keepdims=True)
    tensor_scale = peak / (6.0 * 448.0)
    scale = jnp.maximum(top * (1.0 / (6.0 * tensor_scale)), FLOOR).astype(BF16).astype(F32)
    return rounded(x, jnp.broadcast_to(scale * (2.0 * tensor_scale), x.shape)).reshape(n, cols)


def lane_tops(x):
    top = jnp.abs(x)
    for sh in (1, 2, 4, 8):
        top = jnp.maximum(top, pltpu.roll(top, sh, 1))
    return top


def quantized_lanes(pieces, tops, peak, pick):
    rows = pieces[0].shape[0]
    tensor_scale = peak / (6.0 * 448.0)
    inverse = 1.0 / (6.0 * tensor_scale)
    scales = [jnp.maximum(top * inverse, FLOOR).astype(BF16) for top in tops]
    spread = jnp.dot(jnp.concatenate(scales, axis=0), pick, preferred_element_type=F32)
    return [
        rounded(x, spread[i * rows : (i + 1) * rows] * (2.0 * tensor_scale)) for i, x in enumerate(pieces)
    ]


def pick_matrix():
    src = lax.broadcasted_iota(jnp.int32, (128, 128), 0)
    dst = lax.broadcasted_iota(jnp.int32, (128, 128), 1)
    same = (src // 16 == dst // 16) & (src % 16 == 15)
    return jnp.where(same, 1.0, 0.0).astype(BF16)


class Copies:
    def __init__(self, send_sems, recv_sems, dev):
        self.send_sems, self.recv_sems, self.dev = send_sems, recv_sems, dev
        self.sent, self.n_recv = [], 0

    def copy(self, src, dst, send, recv, dev):
        return pltpu.make_async_remote_copy(
            src_ref=src,
            dst_ref=dst,
            send_sem=self.send_sems.at[send],
            recv_sem=self.recv_sems.at[recv],
            device_id=dev,
            device_id_type=MESH,
        )

    def sender(self, total):
        self.sent.append(total)
        return len(self.sent) - 1

    def receiver(self):
        self.n_recv += 1
        return self.n_recv - 1

    def start(self, src, dst, dev, send, recv):
        self.copy(src, dst, send, recv, dev).start()

    def start_one(self, src, dst, dev, send, landing):
        recv = self.receiver()
        self.start(src, dst, dev, send, recv)
        return lambda: self.arrived(recv, landing)

    def arrived(self, recv, landing):
        self.copy(landing, landing, 0, recv, self.dev).wait_recv()

    def finish(self):
        for i, total in enumerate(self.sent):
            self.copy(total, total, i, 0, self.dev).wait_send()


N_SEND = 13
N_RECV = 74


def kernel(
    q_hbm,
    k_hbm,
    v_hbm,
    w_hbm,
    res_hbm,
    gain_ref,
    hid_ref,
    tops_ref,
    new_ref,
    top_ref,
    q_buf,
    kv_buf,
    w_stage,
    w_raw,
    w_all,
    vt_buf,
    m_ref,
    l_ref,
    o_ref,
    att_buf,
    z_buf,
    act_all,
    out_buf,
    part_buf,
    res_buf,
    hid_buf,
    tiles,
    pick_buf,
    tops_buf,
    new_buf,
    send_sems,
    recv_sems,
    local_sems,
):
    dd, ss, tt = lax.axis_index("dp"), lax.axis_index("seq"), lax.axis_index("tp")
    yy = lax.div(ss, 2)
    cc = ss - 2 * yy

    def sid(dy, dc):
        return lax.rem(yy + dy + 4, 4) * 2 + (cc if dc == 0 else 1 - cc)

    def zt(k):
        return lax.rem(tt + k + 2 * NTP, NTP)

    def sq(k):
        return lax.rem(ss + k + 2 * NSEQ, NSEQ)

    def xd(k):
        return lax.rem(dd + k + 2 * NDP, NDP)

    loads = [
        pltpu.make_async_copy(k_hbm, kv_buf.at[ss, 0], local_sems.at[0]),
        pltpu.make_async_copy(v_hbm, kv_buf.at[ss, 1], local_sems.at[1]),
        pltpu.make_async_copy(q_hbm, q_buf, local_sems.at[2]),
        pltpu.make_async_copy(
            w_hbm.at[:, pl.ds(pl.multiple_of(ss * COLS + dd * SUB, SUB), SUB)],
            w_raw.at[dd],
            local_sems.at[3],
        ),
    ]
    for i in range(4):
        loads.append(
            pltpu.make_async_copy(
                w_hbm.at[pl.ds(i * 128, 128)], w_stage.at[pl.ds(i * 128, 128)], local_sems.at[4 + i]
            )
        )
    loads.append(pltpu.make_async_copy(res_hbm, res_buf, local_sems.at[8]))
    for load in loads:
        load.start()

    barrier = pltpu.get_barrier_semaphore()
    for k in range(1, NTP):
        pl.semaphore_signal(barrier, inc=1, device_id={"tp": zt(k)}, device_id_type=MESH)
    for k in range(1, NSEQ):
        pl.semaphore_signal(barrier, inc=1, device_id={"seq": sq(k)}, device_id_type=MESH)
    for k in (1, 3):
        pl.semaphore_signal(barrier, inc=1, device_id={"dp": xd(k)}, device_id_type=MESH)

    copies = Copies(send_sems, recv_sems, {"tp": zt(1)})
    pick_buf[...] = pick_matrix()

    class SeqGather:
        def __init__(self, unit, half, total):
            self.unit, self.half, self.send = unit, half, copies.sender(total)
            own = unit(sid(0, 0))
            self.x1 = self.go(own, sid(1, 0), unit(sid(-1, 0)))
            self.x2 = self.go(own, sid(-1, 0), unit(sid(1, 0)))
            self.x0 = self.go(own, sid(0, 1), unit(sid(0, 1)))

        def go(self, ref, to, landing):
            return copies.start_one(ref, ref, {"seq": to}, self.send, landing)

        def low(self):
            self.x1()
            got, part = self.unit(sid(-1, 0)), self.half(sid(-1, 0), 0)
            self.x4 = self.go(part, sid(1, 0), self.half(sid(2, 0), 0))
            self.x3 = self.go(got, sid(0, 1), self.unit(sid(-1, 1)))

        def high(self):
            self.x2()
            got, part = self.unit(sid(1, 0)), self.half(sid(1, 0), 1)
            self.x6 = self.go(part, sid(-1, 0), self.half(sid(2, 0), 1))
            self.x5 = self.go(got, sid(0, 1), self.unit(sid(1, 1)))

        def far(self):
            self.x4()
            self.x6()
            self.x7 = self.go(self.unit(sid(2, 0)), sid(0, 1), self.unit(sid(2, 1)))

    def spread_tile(src, dst_of, axis, at):
        me = tt if axis == "tp" else ss
        seven = tiles.at[pl.ds(dst_of, 7)]
        send, recv = copies.sender(seven), copies.receiver()
        for k in range(1, 8):
            copies.start(tiles.at[src], tiles.at[dst_of + me], {axis: at(k)}, send, recv)
        return lambda: copies.arrived(recv, seven)

    def max_of_tiles(first):
        top = tiles[first]
        for i in range(1, 8):
            top = jnp.maximum(top, tiles[first + i])
        return top

    tiles[48] = jnp.zeros((8, 128), F32)
    for i in range(4):
        loads[4 + i].wait()

        @pl.loop(0, 16)
        def _(j, i=i):
            top = tiles[48]
            piece = jnp.abs(w_stage[i * 128 : (i + 1) * 128, pl.ds(pl.multiple_of(j * 512, 512), 512)].astype(F32))
            top4 = jnp.max(piece.reshape(16, 8, 512), axis=0)
            for n in range(4):
                top = jnp.maximum(top, top4[:, n * 128 : (n + 1) * 128])
            tiles[48] = top

    tiles[8 + tt] = tiles[48]
    pl.semaphore_wait(barrier, NTP - 1 + NSEQ - 1 + 2)
    loads[0].wait()
    loads[1].wait()
    kv = SeqGather(lambda i: kv_buf.at[i], lambda i, h: kv_buf.at[i, h], kv_buf.at[pl.ds(0, NSEQ - 1)])

    loads[3].wait()
    raw_send = copies.sender(w_raw.at[pl.ds(0, NDP - 1)])
    raw_far = []

    def raw_go(ref, to, landing):
        return copies.start_one(ref, ref, {"dp": to}, raw_send, landing)

    raw_left = raw_go(w_raw.at[dd], xd(1), w_raw.at[xd(-1)])
    raw_right = raw_go(w_raw.at[dd], xd(-1), w_raw.at[xd(1)])

    def raw_forward():
        for arrival, d, to, rows in (
            (raw_left, xd(-1), xd(1), pl.ds(0, FEAT // 2)),
            (raw_right, xd(1), xd(-1), pl.ds(FEAT // 2, FEAT // 2)),
        ):
            arrival()
            raw_far.append(raw_go(w_raw.at[d, rows], to, w_raw.at[xd(2), rows]))


    w_top = spread_tile(48, 8, "tp", zt)

    def attend(block, kind):
        vt_buf[...] = kv_buf[block, 1].T

        @pl.loop(0, HEADS // PAIR)
        def _(i):
            heads = [i * PAIR + n for n in range(PAIR)]
            scores = [
                lax.dot_general(
                    kv_buf[block, 0],
                    q_buf[:, pl.ds(pl.multiple_of(h * HEAD, HEAD), HEAD)],
                    (((1,), (1,)), ((), ())),
                    preferred_element_type=F32,
                )
                for h in heads
            ]
            for h, sc in zip(heads, scores):
                if kind == "own":
                    key = lax.broadcasted_iota(jnp.int32, (TOK, TOK), 0)
                    query = lax.broadcasted_iota(jnp.int32, (TOK, TOK), 1)
                    sc = jnp.where(key <= query, sc, NEG)
                top = jnp.max(sc, axis=0, keepdims=True)
                if kind != "own":
                    old = m_ref[h]
                    top = jnp.maximum(old, top)
                p = jnp.exp2((sc - top) * SCALE)
                total = jnp.sum(p, axis=0, keepdims=True)
                o = lax.dot_general(
                    vt_buf[...], p.astype(BF16), (((1,), (0,)), ((), ())), preferred_element_type=F32
                )
                if kind != "own":
                    shrink = jnp.exp2((old - top) * SCALE)
                    total = total + l_ref[h] * shrink
                    o = o + o_ref[h] * shrink
                m_ref[h] = top
                l_ref[h] = total
                o_ref[h] = o

    def attend_if_before(block):
        @pl.when(block < ss)
        def _():
            attend(block, "before")

    loads[2].wait()
    attend(ss, "own")

    w_top()
    w_peak = jnp.max(max_of_tiles(8))

    def quantize_weights(d):
        @pl.loop(0, 4)
        def _(i):
            rows = pl.ds(pl.multiple_of(i * 128, 128), 128)
            to = pl.ds(pl.multiple_of(tt * FEAT + i * 128, 128), 128)
            w_all[d, to, :] = quantized_rows(w_raw[d, rows, :].astype(F32), w_peak)

    quantize_weights(dd)

    def unit_a(d, t):
        return w_all.at[d, pl.ds(pl.multiple_of(t * FEAT, 16), RA)]

    def part_a(d, t, low, high):
        return w_all.at[d, pl.ds(pl.multiple_of(t * FEAT + low, 16), high - low)]

    def part_b(t, low, high):
        return w_all.at[:, pl.ds(pl.multiple_of(t * FEAT + low, 16), high - low)]

    rel = (0, -1, 1, -2, 2, -3, 3, -4)
    up = {0: 0, 1: 1, 2: 3, 3: 5, 4: 7}
    down = {0: 0, 1: 2, 2: 4, 3: 6}
    x_left, x_right, x_far, b_up, b_down, a_up, a_down = {}, {}, {}, {}, {}, {}, {}

    w_send = copies.sender(w_all.at[:, pl.ds(0, 28 * FEAT // NDP)])

    def w_go(ref, to, landing):
        return copies.start_one(ref, ref, to, w_send, landing)

    def x_sends(j):
        t_j = zt(rel[j])
        own = unit_a(dd, t_j)
        x_left[j] = w_go(own, {"dp": xd(1)}, unit_a(xd(-1), t_j))
        x_right[j] = w_go(own, {"dp": xd(-1)}, unit_a(xd(1), t_j))

    def a_send_up(step):
        cut = RA // 2 if step == 3 else RA
        landing = part_a(dd, zt(-step - 1), 0, cut)
        a_up[step + 1] = w_go(part_a(dd, zt(-step), 0, cut), {"tp": zt(1)}, landing)

    def a_send_down(step):
        cut = RA // 2 if step == 3 else 0
        landing = part_a(dd, zt(step + 1), cut, RA)
        a_down[step + 1] = w_go(part_a(dd, zt(step), cut, RA), {"tp": zt(-1)}, landing)

    def b_send_up(step):
        cut = (RA + FEAT) // 2 if step == 3 else FEAT
        landing = part_b(zt(-step - 1), RA, cut)
        b_up[step + 1] = w_go(part_b(zt(-step), RA, cut), {"tp": zt(1)}, landing)

    def b_send_down(step):
        cut = (RA + FEAT) // 2 if step == 3 else RA
        landing = part_b(zt(step + 1), cut, FEAT)
        b_down[step + 1] = w_go(part_b(zt(step), cut, FEAT), {"tp": zt(-1)}, landing)

    a_send_up(0)
    a_send_down(0)

    def ev_b0():
        for arrival in raw_far:
            arrival()
        quantize_weights(xd(2))
        b_send_up(0)
        b_send_down(0)

    def ev_a(step):
        a_up[step]()
        if step < 4:
            a_send_up(step)
            x_sends(up[step])
        a_down[step]()
        if step < 4:
            a_send_down(step)
            x_sends(down[step])
        else:
            x_sends(up[step])

    def ev_b(step):
        b_up[step]()
        if step < 4:
            b_send_up(step)
        b_down[step]()
        if step < 4:
            b_send_down(step)

    def ev_x(j):
        def go():
            t_j = zt(rel[j])
            cut = {7: RA // 2}.get(j, RA if j % 2 == 0 else 0)
            x_left[j]()
            x_far[j] = []
            if cut > 0:
                x_far[j].append(w_go(part_a(xd(-1), t_j, 0, cut), {"dp": xd(1)}, part_a(xd(2), t_j, 0, cut)))
            x_right[j]()
            if cut < RA:
                x_far[j].append(w_go(part_a(xd(1), t_j, cut, RA), {"dp": xd(-1)}, part_a(xd(2), t_j, cut, RA)))

        return go

    kv.x0()
    attend_if_before(sid(0, 1))
    kv.low()
    kv.high()
    raw_forward()
    attend_if_before(sid(-1, 0))
    attend_if_before(sid(1, 0))
    kv.x3()
    attend_if_before(sid(-1, 1))
    kv.far()
    ev_a(1)
    quantize_weights(xd(-1))
    quantize_weights(xd(1))
    ev_b0()
    kv.x5()
    attend_if_before(sid(1, 1))
    attend_if_before(sid(2, 0))
    kv.x7()
    attend_if_before(sid(2, 1))

    tiles[49] = jnp.zeros((8, 128), F32)
    for h in range(HEADS):
        a = (o_ref[h] / l_ref[h]).T.astype(BF16)
        att_buf[:, h * HEAD : (h + 1) * HEAD] = a
        tiles[49] = jnp.maximum(tiles[49], jnp.max(jnp.abs(a.astype(F32)).reshape(TOK // 8, 8, HEAD), axis=0))
    tiles[16 + tt] = tiles[49]
    a_top = spread_tile(49, 16, "tp", zt)
    a_moves = []
    for part in range(2):
        seven = z_buf.at[part, pl.ds(0, NTP - 1)]
        send, recv = copies.sender(seven), copies.receiver()
        for k in range(1, NTP):
            copies.start(
                att_buf.at[pl.ds(pl.multiple_of(zt(k) * OWN + part * HALF, HALF), HALF)],
                z_buf.at[part, tt],
                {"tp": zt(k)},
                send,
                recv,
            )
        a_moves.append(lambda recv=recv, seven=seven: copies.arrived(recv, seven))
        z_buf[part, tt] = att_buf[pl.ds(pl.multiple_of(tt * OWN + part * HALF, HALF), HALF), :]
    ev_a(2)
    ev_x(1)()
    a_top()
    tiles[50] = max_of_tiles(16)
    tiles[24 + ss] = tiles[50]
    s_top = spread_tile(50, 24, "seq", sq)
    ev_x(2)()
    ev_b(1)
    s_top()
    a_peak = jnp.max(max_of_tiles(24))
    ev_x(3)()

    acts = []
    for part in range(2):
        a_moves[part]()

        @pl.loop(0, NTP // GROUP)
        def _(i, part=part):
            pieces = [
                z_buf[part, GROUP * i + g, :, n * 128 : (n + 1) * 128].astype(F32)
                for g in range(GROUP)
                for n in range(FEAT // 128)
            ]
            tops = [lane_tops(x) for x in pieces]
            for n, x in enumerate(quantized_lanes(pieces, tops, a_peak, pick_buf[...])):
                act_all[ss, part, :, pl.ds(pl.multiple_of(i * GROUP * FEAT + n * 128, 128), 128)] = x

        acts.append(
            SeqGather(
                lambda i, part=part: act_all.at[i, part],
                lambda i, h, part=part: act_all.at[i, part, pl.ds(h * (HALF // 2), HALF // 2)],
                act_all.at[pl.ds(0, NSEQ - 1), part],
            )
        )
        if part == 0:
            ev_x(4)()

    part_seven = part_buf.at[pl.ds(0, NSEQ - 1)]
    out_send, out_recv = copies.sender(part_seven), copies.receiver()

    def sub_of(i):
        return lax.rem(dd + i + lax.div(i, 2) - 2 * lax.div(i, 3), NDP)

    def project(i, low, high):
        @pl.loop(low, high)
        def _(n):
            chip = lax.rem(yy + 1 + 2 * n - lax.div(n, 2), 4)
            lhs = act_all[pl.ds(chip * 2, 2)].reshape(2 * OWN, NTP * FEAT)
            prod = jnp.dot(lhs, w_all[sub_of(i)], preferred_element_type=F32).astype(BF16)
            out_buf[chip * 2, i] = prod[:OWN]
            out_buf[chip * 2 + 1, i] = prod[OWN:]

        for dy in (1, -1, 0, 2)[low:high]:
            for dc in range(2):
                to = sid(dy, dc)
                if dy == 0 and dc == 0:
                    part_buf[ss, i] = out_buf[ss, i]
                else:
                    copies.start(out_buf.at[to, i], part_buf.at[ss, i], {"seq": to}, out_send, out_recv)

    ev_a(3)
    acts[0].low()
    acts[0].high()
    ev_b(2)
    acts[1].low()
    acts[1].high()
    ev_a(4)
    ev_x(5)()
    acts[0].far()
    ev_b(3)
    acts[1].far()
    ev_x(6)()
    ev_b(4)
    for a in acts:
        for arrival in (a.x0, a.x3, a.x5):
            arrival()
    project(0, 0, 3)
    for a in acts:
        a.x7()
    project(0, 3, 4)
    ev_x(7)()
    project(1, 0, 4)
    project(2, 0, 4)
    for arrivals in x_far.values():
        for arrival in arrivals:
            arrival()
    project(3, 3, 4)
    project(3, 0, 3)
    loads[8].wait()
    copies.arrived(out_recv, part_seven)

    square = jnp.zeros((OWN, 128), F32)
    for i in range(NSEQ):
        for j in range(NDP):
            cols = pl.ds(pl.multiple_of(i * COLS + sub_of(j) * SUB, SUB), SUB)
            hid = res_buf[:, cols].astype(F32) + part_buf[i, j].astype(F32)
            hid_buf[:, cols] = hid
            new_buf[:, cols] = hid.astype(BF16)
            sqr = hid * hid
            for n in range(SUB // 128):
                square = square + sqr[:, n * 128 : (n + 1) * 128]
    stores = [pltpu.make_async_copy(new_buf, new_ref, local_sems.at[9])]
    stores[0].start()
    mean = jnp.sum(square, axis=1, keepdims=True) * (1.0 / D)
    root = lax.rsqrt(mean + 1e-05)
    top = jnp.zeros((OWN, 128), F32)
    for i in range(D // 128):
        cols = slice(i * 128, (i + 1) * 128)
        normed = hid_buf[:, cols] * root * gain_ref[i : i + 1, :].astype(F32)
        hid_buf[:, cols] = normed
        top = jnp.maximum(top, jnp.abs(normed))
    tiles[51] = jnp.max(top.reshape(OWN // 8, 8, 128), axis=0)
    tiles[32 + tt] = tiles[51]
    n_top = spread_tile(51, 32, "tp", zt)
    stores.append(pltpu.make_async_copy(hid_buf, hid_ref, local_sems.at[10]))
    stores[1].start()

    @pl.loop(0, D // 128 // TILES)
    def _(i):
        for n in range(TILES):
            cols = pl.ds(pl.multiple_of((i * TILES + n) * 128, 128), 128)
            tops_buf[:, cols] = lane_tops(hid_buf[:, cols])

    stores.append(pltpu.make_async_copy(tops_buf, tops_ref, local_sems.at[11]))
    stores[2].start()
    n_top()
    tiles[52] = max_of_tiles(32)
    tiles[40 + ss] = tiles[52]
    spread_tile(52, 40, "seq", sq)()
    tiles[53] = max_of_tiles(40)
    stores.append(pltpu.make_async_copy(tiles.at[53], top_ref, local_sems.at[12]))
    stores[3].start()

    assert len(copies.sent) == N_SEND and copies.n_recv == N_RECV
    copies.finish()
    for store in stores:
        store.wait()


STEPS = 4
TILES = 8


def quantize_kernel(hid_ref, tops_ref, sum_ref, top_ref, new_ref, next_ref):
    peak = jnp.max(top_ref[...])
    pick = pick_matrix()

    @pl.loop(0, D // STEPS // 128 // TILES)
    def _(i):
        cols = [pl.ds(pl.multiple_of((i * TILES + n) * 128, 128), 128) for n in range(TILES)]
        pieces = [hid_ref[:, c] for c in cols]
        tops = [tops_ref[:, c] for c in cols]
        for c, x in zip(cols, quantized_lanes(pieces, tops, peak, pick)):
            next_ref[:, c] = x
            new_ref[:, c] = sum_ref[:, c]


def local(queries, keys, values, out_weight, residual, norm_gain):
    any_space = pl.BlockSpec(memory_space=pl.ANY)
    vmem = pl.BlockSpec(memory_space=pltpu.VMEM)
    gain = norm_gain.reshape(D // 128, 128)
    hid, tops, new, top = pl.pallas_call(
        kernel,
        out_shape=(
            jax.ShapeDtypeStruct((OWN, D), F32),
            jax.ShapeDtypeStruct((OWN, D), F32),
            jax.ShapeDtypeStruct((OWN, D), BF16),
            jax.ShapeDtypeStruct((8, 128), F32),
        ),
        in_specs=[any_space] * 5 + [vmem],
        out_specs=(any_space,) * 4,
        scratch_shapes=[
            pltpu.VMEM((TOK, FEAT), BF16),
            pltpu.VMEM((NSEQ, 2, TOK, HEAD), BF16),
            pltpu.VMEM((FEAT, D), BF16),
            pltpu.VMEM((NDP, FEAT, SUB), BF16),
            pltpu.VMEM((NDP, NTP * FEAT, SUB), BF16),
            pltpu.VMEM((HEAD, TOK), BF16),
            pltpu.VMEM((HEADS, 1, TOK), F32),
            pltpu.VMEM((HEADS, 1, TOK), F32),
            pltpu.VMEM((HEADS, HEAD, TOK), F32),
            pltpu.VMEM((TOK, FEAT), BF16),
            pltpu.VMEM((2, NTP, HALF, FEAT), BF16),
            pltpu.VMEM((NSEQ, 2, HALF, NTP * FEAT), BF16),
            pltpu.VMEM((NSEQ, NDP, OWN, SUB), BF16),
            pltpu.VMEM((NSEQ, NDP, OWN, SUB), BF16),
            pltpu.VMEM((OWN, D), BF16),
            pltpu.VMEM((OWN, D), F32),
            pltpu.VMEM((56, 8, 128), F32),
            pltpu.VMEM((128, 128), BF16),
            pltpu.VMEM((OWN, D), F32),
            pltpu.VMEM((OWN, D), BF16),
            pltpu.SemaphoreType.DMA((N_SEND,)),
            pltpu.SemaphoreType.DMA((N_RECV,)),
            pltpu.SemaphoreType.DMA((13,)),
        ],
        compiler_params=pltpu.CompilerParams(
            collective_id=0, has_side_effects=True, vmem_limit_bytes=60 * 1024 * 1024
        ),
    )(queries, keys, values, out_weight, residual, gain)
    out = jax.ShapeDtypeStruct((OWN, D), BF16)
    wide = pl.BlockSpec((OWN, D // STEPS), lambda i: (0, i))
    return pl.pallas_call(
        quantize_kernel,
        grid=(STEPS,),
        out_shape=(out, out),
        in_specs=[wide, wide, wide, pl.BlockSpec((8, 128), lambda i: (0, 0))],
        out_specs=(wide, wide),
    )(hid, tops, new, top)


def solution(mesh):
    in_specs = (
        P(("dp", "seq"), "tp"),
        P(("dp", "seq"), "tp"),
        P(("dp", "seq"), "tp"),
        P("tp", None),
        P(("dp", "seq", "tp"), None),
        P(),
    )
    out_specs = (P(("dp", "seq", "tp"), None), P(("dp", "seq", "tp"), None))
    return jax.shard_map(local, mesh=mesh, in_specs=in_specs, out_specs=out_specs, check_vma=False)
```
